32 devices in a mesh: row: 4 (over z), col: 2 (over x), depth: 4 (over y, core).
Axes of the slice: x: 2, y: 2, z: 4, core: 2. Of those that a mesh axis runs over, the one named last changes fastest.
Arguments:
- pair_input: bfloat16 [192, 192, 128], P('row', ('col', 'depth')), may hold values from -40 to 40
- in_gain: float32 [128], replicated, may hold values from 0.1 to 1.9
- in_shift: float32 [128], replicated, may hold values from -3 to 3
- w_proj: bfloat16 [128, 512], replicated, may hold values from -0.5 to 0.5
- w_gate: bfloat16 [128, 128], replicated, may hold values from -0.5 to 0.5
- out_gain: float32 [128], replicated, may hold values from 0.1 to 1.9
- out_shift: float32 [128], replicated, may hold values from -3 to 3
- w_out: bfloat16 [128, 128], replicated, may hold values from -0.5 to 0.5
Outputs:
- update: bfloat16 [192, 192, 128], P('row', ('col', 'depth'))
The draws below stay inside these ranges and needn't reach their ends.
All inputs are finite; a program needn't handle non-finite values.
Results may differ from the reference program's by a relative error of at most 0.013.
Values may be sent and summed in bfloat16 or wider, within the bound.
A program may use at most 64 MiB of HBM per device.

```python
import math
import jax
import jax.numpy as jnp
from jax import lax

C_Z = 128
C = 128
RESIDUES = 192


def draw_pair_input(key, part):
    key_entries = jax.random.fold_in(key, 11)
    key_scales = jax.random.fold_in(key, 12)
    scales = jnp.exp(jax.random.uniform(key_scales, (RESIDUES, RESIDUES, 1), jnp.float32, 0.0, math.log(10.0)))
    entries = jnp.clip(jax.random.normal(key_entries, (RESIDUES, RESIDUES, C_Z), jnp.float32), -4.0, 4.0)
    values = entries * scales
    return values.astype(jnp.bfloat16)


def gaussian(stream_key, shape, width, most, kind=jnp.bfloat16):
    return jnp.clip(width * jax.random.normal(stream_key, shape, jnp.float32), -most, most).astype(kind)


def setup_inputs(seed: int = 0) -> dict:
    splits = jax.random.split(jax.random.key(seed), 9)
    return {
        "pair_input": draw_pair_input(jax.random.fold_in(splits[8], 71), 0),
        "in_gain": jnp.clip(1.0 + 0.18 * jax.random.normal(splits[1], (C_Z,), jnp.float32), 0.1, 1.9),
        "in_shift": gaussian(splits[2], (C_Z,), 0.5, 3.0, jnp.float32),
        "w_proj": gaussian(splits[3], (C_Z, 4 * C), C_Z ** -0.5, 0.5),
        "w_gate": gaussian(splits[4], (C_Z, C_Z), C_Z ** -0.5, 0.5),
        "out_gain": jnp.clip(1.0 + 0.18 * jax.random.normal(splits[5], (C,), jnp.float32), 0.1, 1.9),
        "out_shift": gaussian(splits[6], (C,), 0.5, 3.0, jnp.float32),
        "w_out": gaussian(splits[7], (C, C_Z), C ** -0.5, 0.5),
    }


def layer_norm(values, scaling, offsets):
    average = lax.optimization_barrier(jnp.mean(values, axis=-1, keepdims=True))
    centred = values - average
    variance = lax.optimization_barrier(jnp.mean(centred * centred, axis=-1, keepdims=True))
    return centred * lax.rsqrt(variance + 1e-05) * scaling + offsets

def reference(pair_input, in_gain, in_shift, w_proj, w_gate, out_gain, out_shift, w_out):
    normed = layer_norm(pair_input.astype(jnp.float32), in_gain, in_shift).astype(jnp.bfloat16)
    channels = w_proj.shape[1] // 4

    def side_rows(normed_row):
        projected = jnp.dot(normed_row, w_proj, preferred_element_type=jnp.float32)
        left_side = (jax.nn.sigmoid(projected[:, :channels]) * projected[:, channels:2 * channels]).astype(jnp.bfloat16)
        right_side = (jax.nn.sigmoid(projected[:, 2 * channels:3 * channels]) * projected[:, 3 * channels:]).astype(jnp.bfloat16)
        return (left_side, right_side)
    left_side, right_side = lax.map(side_rows, normed)
    product = jnp.einsum('kic,kjc->ijc', left_side.astype(jnp.float32), right_side.astype(jnp.float32), precision=lax.Precision.HIGHEST)
    product_norm = layer_norm(product, out_gain, out_shift).astype(jnp.bfloat16)
    gating = jax.nn.sigmoid(jnp.einsum('xyc,cd->xyd', normed.astype(jnp.float32), w_gate.astype(jnp.float32), precision=lax.Precision.HIGHEST))
    projected_out = jnp.einsum('xyc,cd->xyd', product_norm.astype(jnp.float32), w_out.astype(jnp.float32), precision=lax.Precision.HIGHEST)
    return (gating * projected_out).astype(jnp.bfloat16)
```

```python
import functools

import jax
import jax.numpy as jnp
from jax import lax
from jax.experimental import pallas as pl
from jax.experimental.pallas import tpu as pltpu
from jax.sharding import PartitionSpec as P

F32 = jnp.float32
BF16 = jnp.bfloat16
MESH = pl.DeviceIdType.MESH
LANES = 128
SUB = 8
WIDE = LANES // SUB
UNROLL = 64


def dot(a, b, ca, cb):
    return lax.dot_general(a, b, (((ca,), (cb,)), ((), ())), preferred_element_type=F32)


def repeat(n, body):
    if n <= UNROLL:
        for i in range(n):
            body(i)
    else:
        lax.fori_loop(0, n, lambda i, carry: (body(i), carry)[1], 0)


def block_transpose(arrays, block, lane):
    arrays = list(arrays)
    lanes = arrays[0].shape[1]
    for d in (4, 2, 1):
        low = (lane // block) & d == 0
        for a in range(SUB):
            if a & d:
                continue
            x, y = arrays[a], arrays[a | d]
            if y is None:
                arrays[a] = jnp.where(low, x, 0.0)
                arrays[a | d] = jnp.where(low, pltpu.roll(x, lanes - d * block, 1), 0.0)
            else:
                arrays[a] = jnp.where(low, x, pltpu.roll(y, d * block, 1))
                arrays[a | d] = jnp.where(low, pltpu.roll(x, lanes - d * block, 1), y)
    return arrays


def kernel(
    plan,
    x_ref,
    in_gain_ref,
    in_shift_ref,
    w_proj_ref,
    w_gate_ref,
    out_gain_ref,
    out_shift_ref,
    w_out_ref,
    out_ref,
    normed,
    w_turned,
    gating,
    packed,
    send1,
    recv1,
    gathered,
    left_rows,
    right_rows,
    planes,
    send2,
    recv2,
    gathered2,
    turned,
    send_sem1,
    recv_sem1,
    send_sem2,
    recv_sem2,
):
    rows, cols, depths, parts, chunks = plan
    others = cols * depths
    count = rows * others
    local_k, local_i, width = x_ref.shape
    hidden = w_out_ref.shape[0]
    part_rows = rows // parts
    members = part_rows * others
    each = hidden // members // chunks
    part_hidden = hidden // chunks
    groups = local_i // SUB
    deep = local_k // WIDE
    tiles = deep * groups
    pairs = local_k // local_i // 2
    span1 = each * 2 * tiles
    spots = groups * groups
    span2 = spots * pairs * each
    slabs = part_rows * deep
    slab_tiles = -(-slabs // SUB)
    line = groups * others

    my_row = lax.axis_index("row")
    my_other = lax.axis_index("col") * depths + lax.axis_index("depth")
    me = my_row * others + my_other
    my_part = lax.div(me, members)
    my_slot = lax.rem(me, members)
    part_base = my_part * members

    def device(p):
        q = lax.rem(p, others)
        return (lax.div(p, others), lax.div(q, depths), lax.rem(q, depths))

    barrier = pltpu.get_barrier_semaphore()

    def greet(d):
        pl.semaphore_signal(
            barrier, inc=1, device_id=device(lax.rem(me + d + 1, count)), device_id_type=MESH
        )

    repeat(count - 1, greet)

    values = x_ref[...].astype(F32)
    centred = values - jnp.mean(values, axis=-1, keepdims=True)
    variance = jnp.mean(centred * centred, axis=-1, keepdims=True)
    normed[...] = (
        centred * lax.rsqrt(variance + 1e-05) * in_gain_ref[...].reshape(1, 1, width)
        + in_shift_ref[...].reshape(1, 1, width)
    ).reshape(local_k * local_i, width)
    w_turned[...] = w_proj_ref[...].astype(F32).T.astype(BF16)

    def edge_block(kg, ig):
        return jnp.concatenate(
            [
                normed[pl.ds(kg * WIDE * local_i + ig * SUB + i, WIDE, stride=local_i), :]
                for i in range(SUB)
            ],
            axis=0,
        ).astype(BF16)

    def gate_block(pair, first, second):
        return jnp.concatenate(
            [
                normed[pl.ds(((2 * pair + b) * local_i + first * SUB + i) * local_i + second * SUB, SUB), :]
                for b in range(2)
                for i in range(SUB)
            ],
            axis=0,
        ).astype(BF16)

    def project(h):
        for t in range(tiles):
            block = edge_block(t // groups, t % groups)
            for side in range(2):
                start = 2 * side * hidden + h * part_hidden
                gates = dot(w_turned[pl.ds(start, part_hidden), :], block, 1, 1)
                edges = dot(w_turned[pl.ds(start + hidden, part_hidden), :], block, 1, 1)
                packed[pl.ds(side * tiles + t, part_hidden, stride=2 * tiles), :] = (
                    jax.nn.sigmoid(gates) * edges
                )

        def pack(s):
            send1[h, s] = packed[pl.ds(s * span1, span1), :].reshape(send1.shape[2:]).astype(BF16)

        repeat(members, pack)

    def copy1(h, s, slot):
        return pltpu.make_async_remote_copy(
            src_ref=send1.at[h, s],
            dst_ref=recv1.at[h, slot],
            send_sem=send_sem1.at[h],
            recv_sem=recv_sem1.at[h],
            device_id=device(part_base + s),
            device_id_type=MESH,
        )

    def all1(h):
        some = pl.ds(0, members - 1)
        return pltpu.make_async_remote_copy(
            src_ref=send1.at[h, some],
            dst_ref=recv1.at[h, some],
            send_sem=send_sem1.at[h],
            recv_sem=recv_sem1.at[h],
            device_id=device(me),
            device_id_type=MESH,
        )

    def copy2(h, p):
        return pltpu.make_async_remote_copy(
            src_ref=send2.at[h, p],
            dst_ref=recv2.at[h, me],
            send_sem=send_sem2.at[h],
            recv_sem=recv_sem2.at[h],
            device_id=device(p),
            device_id_type=MESH,
        )

    def all2(h):
        some = pl.ds(0, count - 1)
        return pltpu.make_async_remote_copy(
            src_ref=send2.at[h, some],
            dst_ref=recv2.at[h, some],
            send_sem=send_sem2.at[h],
            recv_sem=recv_sem2.at[h],
            device_id=device(me),
            device_id_type=MESH,
        )

    for h in range(chunks):
        project(h)
        if h == 0:
            pl.semaphore_wait(barrier, count - 1)
        repeat(members - 1, lambda d, h=h: copy1(h, lax.rem(my_slot + d + 1, members), my_slot).start())
        recv1[h, my_slot] = send1[h, my_slot]

    for t in range(pairs * groups * groups):
        pair, rest = t // (groups * groups), t % (groups * groups)
        gating[t] = jax.nn.sigmoid(
            dot(gate_block(pair, rest // groups, rest % groups), w_gate_ref[...], 1, 0)
        )
    lane = lax.broadcasted_iota(jnp.int32, (line, LANES), 1)
    small_lane = lax.broadcasted_iota(jnp.int32, (SUB, LANES), 1)

    def order(values):
        turned[...] = values
        return jnp.concatenate(
            [
                turned[pl.ds(h * part_hidden + c, members, stride=each), :]
                for h in range(chunks)
                for c in range(each)
            ],
            axis=0,
        )

    def middle(h):
        all1(h).wait_recv()

        def take(s):
            gathered[pl.ds(s * span1, span1), :] = recv1[h, s].astype(F32).reshape(span1, LANES)

        repeat(members, take)
        half = SUB * line // 2
        for c in range(each):
            for side in range(2):
                for kt in range(slab_tiles):
                    arrays = []
                    for kb in range(kt * SUB, kt * SUB + SUB):
                        if kb >= slabs:
                            arrays.append(None)
                            continue
                        start = (
                            (kb // deep) * others * span1
                            + (c * 2 + side) * tiles
                            + (kb % deep) * groups
                        )
                        arrays.append(
                            jnp.concatenate(
                                [
                                    gathered[pl.ds(start + g, others, stride=span1), :]
                                    for g in range(groups)
                                ],
                                axis=0,
                            )
                        )
                    turned_blocks = block_transpose(arrays, WIDE, lane)
                    for i in range(SUB):
                        if side == 0:
                            left_rows[kt, pl.ds(i * line, line), :] = turned_blocks[i]
                        else:
                            right_rows[kt, pl.ds(i, line, stride=SUB), :] = turned_blocks[i]
            left = jnp.concatenate(
                [left_rows[kt, pl.ds(b, half, stride=2), :] for b in range(2) for kt in range(slab_tiles)],
                axis=1,
            ).astype(BF16)
            wide = SUB * SUB

            def multiply(j, c=c, left=left):
                right = jnp.concatenate(
                    [right_rows[kt, pl.ds(j * wide, wide), :] for kt in range(slab_tiles)], axis=1
                ).astype(BF16)
                empty = jnp.zeros_like(right)
                both = jnp.concatenate(
                    [jnp.concatenate([right, empty], axis=1), jnp.concatenate([empty, right], axis=1)],
                    axis=0,
                )
                planes[j, pl.ds(c, half, stride=each), :] = dot(left, both, 1, 1)

            repeat(line // SUB, multiply)

        stretch = groups * rows * pairs * each
        unit = pairs * each

        def flatten(j):
            g, q = (j // (others // SUB), j % (others // SUB)) if isinstance(j, int) else (
                lax.div(j, others // SUB),
                lax.rem(j, others // SUB),
            )
            for part in range(stretch // SUB):
                arrays = [planes[j, pl.ds(i * stretch + part * SUB, SUB), :] for i in range(SUB)]
                flat = block_transpose(arrays, SUB, small_lane)
                for n in range(SUB // unit):
                    where = part * (SUB // unit) + n
                    first, r = where // rows, where % rows
                    for o in range(SUB):
                        send2[h, r * others + q * SUB + o, g * groups + first] = flat[o][
                            n * unit : (n + 1) * unit
                        ].astype(BF16)

        repeat(line // SUB, flatten)
        repeat(count - 1, lambda d: copy2(h, lax.rem(me + d + 1, count)).start())
        recv2[h, me] = send2[h, me]

    for h in range(chunks):
        middle(h)
    out_gain = order(jnp.broadcast_to(out_gain_ref[...].reshape(1, hidden), (LANES, hidden)).T)
    out_shift = order(jnp.broadcast_to(out_shift_ref[...].reshape(1, hidden), (LANES, hidden)).T)
    w_out = order(w_out_ref[...].astype(F32)).astype(BF16)
    for h in range(chunks):
        all2(h).wait_recv()

        def take2(s, h=h):
            total = recv2[h, s].astype(F32)
            for part in range(1, parts):
                total = total + recv2[h, part * members + s].astype(F32)
            gathered2[pl.ds((h * members + s) * span2, span2), :] = total.reshape(span2, LANES)

        repeat(members, take2)

    for t in range(pairs * groups * groups):
        pair, rest = t // (groups * groups), t % (groups * groups)
        first, second = rest // groups, rest % groups
        start = (second * groups + first) * pairs * each + pair * each
        product = jnp.concatenate(
            [
                gathered2[pl.ds(h * members * span2 + start + c, members, stride=span2), :]
                for h in range(chunks)
                for c in range(each)
            ],
            axis=0,
        )
        spread_out = product - jnp.mean(product, axis=0, keepdims=True)
        moment = jnp.mean(spread_out * spread_out, axis=0, keepdims=True)
        product_norm = (spread_out * lax.rsqrt(moment + 1e-05) * out_gain + out_shift).astype(BF16)
        update = (gating[t] * dot(product_norm, w_out, 0, 0)).astype(BF16)
        for b in range(2):
            out_ref[
                pl.ds((2 * pair + b) * local_i + first * SUB, SUB), pl.ds(second * SUB, SUB), :
            ] = update[b * SUB * SUB : (b + 1) * SUB * SUB].reshape(SUB, SUB, width)

    for h in range(chunks):
        all1(h).wait_send()
        all2(h).wait_send()


def per_device(sizes, pair_input, in_gain, in_shift, w_proj, w_gate, out_gain, out_shift, w_out):
    rows, cols, depths = sizes
    parts, chunks = 2, 2
    others = cols * depths
    count = rows * others
    local_k, local_i, width = pair_input.shape
    hidden = w_out.shape[0]
    members = count // parts
    each = hidden // members // chunks
    groups = local_i // SUB
    tiles = local_k * local_i // LANES
    span1 = each * 2 * tiles
    line = groups * others
    pairs = local_k // local_i // 2
    unit = pairs * each
    spots = groups * groups
    slab_tiles = -(-(rows // parts * local_k) // LANES)
    vmem = pl.BlockSpec(memory_space=pltpu.VMEM)
    return pl.pallas_call(
        functools.partial(kernel, (rows, cols, depths, parts, chunks)),
        out_shape=jax.ShapeDtypeStruct(pair_input.shape, BF16),
        in_specs=[vmem] * 8,
        out_specs=vmem,
        scratch_shapes=[
            pltpu.VMEM((local_k * local_i, width), F32),
            pltpu.VMEM(w_proj.shape[::-1], BF16),
            pltpu.VMEM((tiles, LANES, width), F32),
            pltpu.VMEM((hidden // chunks * 2 * tiles, LANES), F32),
            pltpu.VMEM((chunks, members, span1 // SUB, SUB, LANES), BF16),
            pltpu.VMEM((chunks, members, span1 // SUB, SUB, LANES), BF16),
            pltpu.VMEM((members * span1, LANES), F32),
            pltpu.VMEM((slab_tiles, SUB * line, LANES), F32),
            pltpu.VMEM((slab_tiles, SUB * line, LANES), F32),
            pltpu.VMEM((line // SUB, SUB * line // 2 * each, LANES), F32),
            pltpu.VMEM((chunks, count, spots, unit, LANES), BF16),
            pltpu.VMEM((chunks, count, spots, unit, LANES), BF16),
            pltpu.VMEM((chunks * members * spots * unit, LANES), F32),
            pltpu.VMEM((hidden, LANES), F32),
            pltpu.SemaphoreType.DMA((chunks,)),
            pltpu.SemaphoreType.DMA((chunks,)),
            pltpu.SemaphoreType.DMA((chunks,)),
            pltpu.SemaphoreType.DMA((chunks,)),
        ],
        compiler_params=pltpu.CompilerParams(
            collective_id=0, has_side_effects=True, vmem_limit_bytes=67_000_000
        ),
    )(
        pair_input,
        in_gain.reshape(1, -1),
        in_shift.reshape(1, -1),
        w_proj,
        w_gate,
        out_gain.reshape(1, -1),
        out_shift.reshape(1, -1),
        w_out,
    )


def solution(mesh):
    sizes = (mesh.shape["row"], mesh.shape["col"], mesh.shape["depth"])
    placed = (P("row", ("col", "depth"), None), P(), P(), P(), P(), P(), P(), P())
    return jax.shard_map(
        functools.partial(per_device, sizes),
        mesh=mesh,
        in_specs=placed,
        out_specs=P("row", ("col", "depth"), None),
        check_vma=False,
    )
```

```python
import functools

import jax
import jax.numpy as jnp
from jax import lax
from jax.experimental import pallas as pl
from jax.experimental.pallas import tpu as pltpu
from jax.sharding import PartitionSpec as P

F32 = jnp.float32
BF16 = jnp.bfloat16
MESH = pl.DeviceIdType.MESH
LANES = 128
SUB = 8
WIDE = LANES // SUB
UNROLL = 64


def dot(a, b, ca, cb):
    return lax.dot_general(a, b, (((ca,), (cb,)), ((), ())), preferred_element_type=F32)


def repeat(n, body):
    if n <= UNROLL:
        for i in range(n):
            body(i)
    else:
        lax.fori_loop(0, n, lambda i, carry: (body(i), carry)[1], 0)


def block_transpose(arrays, block, lane):
    arrays = list(arrays)
    lanes = arrays[0].shape[1]
    for d in (4, 2, 1):
        low = (lane // block) & d == 0
        for a in range(SUB):
            if a & d:
                continue
            x, y = arrays[a], arrays[a | d]
            if y is None:
                arrays[a] = jnp.where(low, x, 0.0)
                arrays[a | d] = jnp.where(low, pltpu.roll(x, lanes - d * block, 1), 0.0)
            else:
                arrays[a] = jnp.where(low, x, pltpu.roll(y, d * block, 1))
                arrays[a | d] = jnp.where(low, pltpu.roll(x, lanes - d * block, 1), y)
    return arrays


def kernel(
    plan,
    x_far,
    w_proj_far,
    in_gain_far,
    in_shift_far,
    w_gate_far,
    out_gain_far,
    out_shift_far,
    w_out_far,
    out_ref,
    x_ref,
    w_proj_ref,
    in_gain_ref,
    in_shift_ref,
    w_gate_ref,
    out_gain_ref,
    out_shift_ref,
    w_out_ref,
    load_sem,
    normed,
    w_turned,
    gating,
    packed,
    send1,
    recv1,
    gathered,
    left_rows,
    right_rows,
    planes,
    send2,
    recv2,
    gathered2,
    turned,
    send_sem1,
    recv_sem1,
    send_sem2,
    recv_sem2,
):
    rows, cols, depths, parts, chunks = plan
    others = cols * depths
    count = rows * others
    local_k, local_i, width = x_ref.shape
    hidden = w_out_ref.shape[0]
    part_rows = rows // parts
    members = part_rows * others
    each = hidden // members // chunks
    part_hidden = hidden // chunks
    groups = local_i // SUB
    deep = local_k // WIDE
    tiles = deep * groups
    pairs = local_k // local_i // 2
    span1 = each * 2 * tiles
    spots = groups * groups
    span2 = spots * pairs * each
    slabs = part_rows * deep
    slab_tiles = -(-slabs // SUB)
    line = groups * others

    my_row = lax.axis_index("row")
    my_other = lax.axis_index("col") * depths + lax.axis_index("depth")
    me = my_row * others + my_other
    my_part = lax.div(me, members)
    my_slot = lax.rem(me, members)
    part_base = my_part * members

    def device(p):
        q = lax.rem(p, others)
        return (lax.div(p, others), lax.div(q, depths), lax.rem(q, depths))

    loads = [
        pltpu.make_async_copy(far, near, load_sem.at[n])
        for n, (far, near) in enumerate(
            (
                (x_far, x_ref),
                (w_proj_far, w_proj_ref),
                (in_gain_far, in_gain_ref),
                (in_shift_far, in_shift_ref),
                (w_gate_far, w_gate_ref),
                (out_gain_far, out_gain_ref),
                (out_shift_far, out_shift_ref),
                (w_out_far, w_out_ref),
            )
        )
    ]
    for load in loads:
        load.start()
    barrier = pltpu.get_barrier_semaphore()

    def greet(d):
        pl.semaphore_signal(
            barrier, inc=1, device_id=device(lax.rem(me + d + 1, count)), device_id_type=MESH
        )

    repeat(count - 1, greet)

    loads[1].wait()
    w_turned[...] = w_proj_ref[...].astype(F32).T.astype(BF16)
    for n in (0, 2, 3):
        loads[n].wait()
    values = x_ref[...].astype(F32)
    centred = values - jnp.mean(values, axis=-1, keepdims=True)
    variance = jnp.mean(centred * centred, axis=-1, keepdims=True)
    normed[...] = (
        centred * lax.rsqrt(variance + 1e-05) * in_gain_ref[...].reshape(1, 1, width)
        + in_shift_ref[...].reshape(1, 1, width)
    ).reshape(local_k * local_i, width)

    def edge_block(kg, ig):
        return jnp.concatenate(
            [
                normed[pl.ds(kg * WIDE * local_i + ig * SUB + i, WIDE, stride=local_i), :]
                for i in range(SUB)
            ],
            axis=0,
        ).astype(BF16)

    def gate_block(pair, first, second):
        return jnp.concatenate(
            [
                normed[pl.ds(((2 * pair + b) * local_i + first * SUB + i) * local_i + second * SUB, SUB), :]
                for b in range(2)
                for i in range(SUB)
            ],
            axis=0,
        ).astype(BF16)

    def project(h):
        for t in range(tiles):
            block = edge_block(t // groups, t % groups)
            for side in range(2):
                start = 2 * side * hidden + h * part_hidden
                gates = dot(w_turned[pl.ds(start, part_hidden), :], block, 1, 1)
                edges = dot(w_turned[pl.ds(start + hidden, part_hidden), :], block, 1, 1)
                packed[pl.ds(side * tiles + t, part_hidden, stride=2 * tiles), :] = (
                    jax.nn.sigmoid(gates) * edges
                )

        def pack(s):
            send1[h, s] = packed[pl.ds(s * span1, span1), :].reshape(send1.shape[2:]).astype(BF16)

        repeat(members, pack)

    def copy1(h, s, slot):
        return pltpu.make_async_remote_copy(
            src_ref=send1.at[h, s],
            dst_ref=recv1.at[h, slot],
            send_sem=send_sem1.at[h],
            recv_sem=recv_sem1.at[h],
            device_id=device(part_base + s),
            device_id_type=MESH,
        )

    def all1(h):
        some = pl.ds(0, members - 1)
        return pltpu.make_async_remote_copy(
            src_ref=send1.at[h, some],
            dst_ref=recv1.at[h, some],
            send_sem=send_sem1.at[h],
            recv_sem=recv_sem1.at[h],
            device_id=device(me),
            device_id_type=MESH,
        )

    def copy2(h, p):
        return pltpu.make_async_remote_copy(
            src_ref=send2.at[h, p],
            dst_ref=recv2.at[h, me],
            send_sem=send_sem2.at[h],
            recv_sem=recv_sem2.at[h],
            device_id=device(p),
            device_id_type=MESH,
        )

    def all2(h):
        some = pl.ds(0, count - 1)
        return pltpu.make_async_remote_copy(
            src_ref=send2.at[h, some],
            dst_ref=recv2.at[h, some],
            send_sem=send_sem2.at[h],
            recv_sem=recv_sem2.at[h],
            device_id=device(me),
            device_id_type=MESH,
        )

    for h in range(chunks):
        project(h)
        if h == 0:
            pl.semaphore_wait(barrier, count - 1)
        repeat(members - 1, lambda d, h=h: copy1(h, lax.rem(my_slot + d + 1, members), my_slot).start())
        recv1[h, my_slot] = send1[h, my_slot]

    for load in loads[4:]:
        load.wait()
    for t in range(pairs * groups * groups):
        pair, rest = t // (groups * groups), t % (groups * groups)
        gating[t] = jax.nn.sigmoid(
            dot(gate_block(pair, rest // groups, rest % groups), w_gate_ref[...], 1, 0)
        )
    lane = lax.broadcasted_iota(jnp.int32, (line, LANES), 1)
    small_lane = lax.broadcasted_iota(jnp.int32, (SUB, LANES), 1)

    def order(values):
        turned[...] = values
        return jnp.concatenate(
            [
                turned[pl.ds(h * part_hidden + c, members, stride=each), :]
                for h in range(chunks)
                for c in range(each)
            ],
            axis=0,
        )

    def middle(h):
        all1(h).wait_recv()

        def take(s):
            gathered[pl.ds(s * span1, span1), :] = recv1[h, s].astype(F32).reshape(span1, LANES)

        repeat(members, take)
        half = SUB * line // 2
        for c in range(each):
            for side in range(2):
                for kt in range(slab_tiles):
                    arrays = []
                    for kb in range(kt * SUB, kt * SUB + SUB):
                        if kb >= slabs:
                            arrays.append(None)
                            continue
                        start = (
                            (kb // deep) * others * span1
                            + (c * 2 + side) * tiles
                            + (kb % deep) * groups
                        )
                        arrays.append(
                            jnp.concatenate(
                                [
                                    gathered[pl.ds(start + g, others, stride=span1), :]
                                    for g in range(groups)
                                ],
                                axis=0,
                            )
                        )
                    turned_blocks = block_transpose(arrays, WIDE, lane)
                    for i in range(SUB):
                        if side == 0:
                            left_rows[kt, pl.ds(i * line, line), :] = turned_blocks[i]
                        else:
                            right_rows[kt, pl.ds(i, line, stride=SUB), :] = turned_blocks[i]
            left = jnp.concatenate(
                [left_rows[kt, pl.ds(b, half, stride=2), :] for b in range(2) for kt in range(slab_tiles)],
                axis=1,
            ).astype(BF16)
            wide = SUB * SUB

            def multiply(j, c=c, left=left):
                right = jnp.concatenate(
                    [right_rows[kt, pl.ds(j * wide, wide), :] for kt in range(slab_tiles)], axis=1
                ).astype(BF16)
                empty = jnp.zeros_like(right)
                both = jnp.concatenate(
                    [jnp.concatenate([right, empty], axis=1), jnp.concatenate([empty, right], axis=1)],
                    axis=0,
                )
                planes[j, pl.ds(c, half, stride=each), :] = dot(left, both, 1, 1)

            repeat(line // SUB, multiply)

        stretch = groups * rows * pairs * each
        unit = pairs * each

        def flatten(j):
            g, q = (j // (others // SUB), j % (others // SUB)) if isinstance(j, int) else (
                lax.div(j, others // SUB),
                lax.rem(j, others // SUB),
            )
            for part in range(stretch // SUB):
                arrays = [planes[j, pl.ds(i * stretch + part * SUB, SUB), :] for i in range(SUB)]
                flat = block_transpose(arrays, SUB, small_lane)
                for n in range(SUB // unit):
                    where = part * (SUB // unit) + n
                    first, r = where // rows, where % rows
                    for o in range(SUB):
                        send2[h, r * others + q * SUB + o, g * groups + first] = flat[o][
                            n * unit : (n + 1) * unit
                        ].astype(BF16)

        repeat(line // SUB, flatten)
        repeat(count - 1, lambda d: copy2(h, lax.rem(me + d + 1, count)).start())
        recv2[h, me] = send2[h, me]

    for h in range(chunks):
        middle(h)
    out_gain = order(jnp.broadcast_to(out_gain_ref[...].reshape(1, hidden), (LANES, hidden)).T)
    out_shift = order(jnp.broadcast_to(out_shift_ref[...].reshape(1, hidden), (LANES, hidden)).T)
    w_out = order(w_out_ref[...].astype(F32)).astype(BF16)
    for h in range(chunks):
        all2(h).wait_recv()

        def take2(s, h=h):
            total = recv2[h, s].astype(F32)
            for part in range(1, parts):
                total = total + recv2[h, part * members + s].astype(F32)
            gathered2[pl.ds((h * members + s) * span2, span2), :] = total.reshape(span2, LANES)

        repeat(members, take2)

    for t in range(pairs * groups * groups):
        pair, rest = t // (groups * groups), t % (groups * groups)
        first, second = rest // groups, rest % groups
        start = (second * groups + first) * pairs * each + pair * each
        product = jnp.concatenate(
            [
                gathered2[pl.ds(h * members * span2 + start + c, members, stride=span2), :]
                for h in range(chunks)
                for c in range(each)
            ],
            axis=0,
        )
        spread_out = product - jnp.mean(product, axis=0, keepdims=True)
        moment = jnp.mean(spread_out * spread_out, axis=0, keepdims=True)
        product_norm = (spread_out * lax.rsqrt(moment + 1e-05) * out_gain + out_shift).astype(BF16)
        update = (gating[t] * dot(product_norm, w_out, 0, 0)).astype(BF16)
        for b in range(2):
            out_ref[
                pl.ds((2 * pair + b) * local_i + first * SUB, SUB), pl.ds(second * SUB, SUB), :
            ] = update[b * SUB * SUB : (b + 1) * SUB * SUB].reshape(SUB, SUB, width)

    for h in range(chunks):
        all1(h).wait_send()
        all2(h).wait_send()


def per_device(sizes, pair_input, in_gain, in_shift, w_proj, w_gate, out_gain, out_shift, w_out):
    rows, cols, depths = sizes
    parts, chunks = 2, 2
    others = cols * depths
    count = rows * others
    local_k, local_i, width = pair_input.shape
    hidden = w_out.shape[0]
    members = count // parts
    each = hidden // members // chunks
    groups = local_i // SUB
    tiles = local_k * local_i // LANES
    span1 = each * 2 * tiles
    line = groups * others
    pairs = local_k // local_i // 2
    unit = pairs * each
    spots = groups * groups
    slab_tiles = -(-(rows // parts * local_k) // LANES)
    operands = (
        pair_input,
        w_proj,
        in_gain.reshape(1, -1),
        in_shift.reshape(1, -1),
        w_gate,
        out_gain.reshape(1, -1),
        out_shift.reshape(1, -1),
        w_out,
    )
    scratch = [
        *(pltpu.VMEM(a.shape, a.dtype) for a in operands),
        pltpu.SemaphoreType.DMA((len(operands),)),
        pltpu.VMEM((local_k * local_i, width), F32),
        pltpu.VMEM(w_proj.shape[::-1], BF16),
        pltpu.VMEM((tiles, LANES, width), F32),
        pltpu.VMEM((hidden // chunks * 2 * tiles, LANES), F32),
        pltpu.VMEM((chunks, members, span1 // SUB, SUB, LANES), BF16),
        pltpu.VMEM((chunks, members, span1 // SUB, SUB, LANES), BF16),
        pltpu.VMEM((members * span1, LANES), F32),
        pltpu.VMEM((slab_tiles, SUB * line, LANES), F32),
        pltpu.VMEM((slab_tiles, SUB * line, LANES), F32),
        pltpu.VMEM((line // SUB, SUB * line // 2 * each, LANES), F32),
        pltpu.VMEM((chunks, count, spots, unit, LANES), BF16),
        pltpu.VMEM((chunks, count, spots, unit, LANES), BF16),
        pltpu.VMEM((chunks * members * spots * unit, LANES), F32),
        pltpu.VMEM((hidden, LANES), F32),
        pltpu.SemaphoreType.DMA((chunks,)),
        pltpu.SemaphoreType.DMA((chunks,)),
        pltpu.SemaphoreType.DMA((chunks,)),
        pltpu.SemaphoreType.DMA((chunks,)),
    ]
    return pl.pallas_call(
        functools.partial(kernel, (rows, cols, depths, parts, chunks)),
        out_shape=pltpu.VMEM(pair_input.shape, BF16),
        in_specs=[pl.BlockSpec(memory_space=pltpu.HBM)] * len(operands),
        out_specs=pl.BlockSpec(memory_space=pltpu.VMEM),
        scratch_shapes=scratch,
        compiler_params=pltpu.CompilerParams(
            collective_id=0, has_side_effects=True, vmem_limit_bytes=60_000_000
        ),
    )(*(pltpu.with_memory_space_constraint(a, pltpu.HBM) for a in operands))


def solution(mesh):
    sizes = (mesh.shape["row"], mesh.shape["col"], mesh.shape["depth"])
    placed = (P("row", ("col", "depth"), None), P(), P(), P(), P(), P(), P(), P())
    return jax.shard_map(
        functools.partial(per_device, sizes),
        mesh=mesh,
        in_specs=placed,
        out_specs=P("row", ("col", "depth"), None),
        check_vma=False,
    )
```

```python
import functools

import jax
import jax.numpy as jnp
from jax import lax
from jax.experimental import pallas as pl
from jax.experimental.pallas import tpu as pltpu
from jax.sharding import PartitionSpec as P

F32 = jnp.float32
BF16 = jnp.bfloat16
MESH = pl.DeviceIdType.MESH
LANES = 128
SUB = 8
WIDE = LANES // SUB
UNROLL = 64
SIZES = (2, 2, 4)
AHEAD = 3


def dot(a, b, ca, cb):
    return lax.dot_general(a, b, (((ca,), (cb,)), ((), ())), preferred_element_type=F32)


def repeat(n, body):
    if n <= UNROLL:
        for i in range(n):
            body(i)
    else:
        lax.fori_loop(0, n, lambda i, carry: (body(i), carry)[1], 0)


def block_transpose(arrays, block, lane):
    arrays = list(arrays)
    lanes = arrays[0].shape[1]
    for d in (4, 2, 1):
        low = (lane // block) & d == 0
        for a in range(SUB):
            if a & d:
                continue
            x, y = arrays[a], arrays[a | d]
            if y is None:
                arrays[a] = jnp.where(low, x, 0.0)
                arrays[a | d] = jnp.where(low, pltpu.roll(x, lanes - d * block, 1), 0.0)
            else:
                arrays[a] = jnp.where(low, x, pltpu.roll(y, d * block, 1))
                arrays[a | d] = jnp.where(low, pltpu.roll(x, lanes - d * block, 1), y)
    return arrays


def kernel(
    plan,
    x_far,
    w_proj_far,
    in_gain_far,
    in_shift_far,
    w_gate_far,
    out_gain_far,
    out_shift_far,
    w_out_far,
    out_ref,
    x_ref,
    w_proj_ref,
    in_gain_ref,
    in_shift_ref,
    w_gate_ref,
    out_gain_ref,
    out_shift_ref,
    w_out_ref,
    load_sem,
    ready,
    normed,
    w_turned,
    gating,
    packed,
    gathered,
    left_rows,
    right_rows,
    planes,
    gathered2,
    turned,
    sems,
    *boxes,
):
    rows, cols, depths, parts, sizes, ahead = plan
    chunks = len(sizes)
    send1, recv1, send2, recv2 = (boxes[n * chunks : (n + 1) * chunks] for n in range(4))
    others = cols * depths
    count = rows * others
    local_k, local_i, width = x_ref.shape
    hidden = w_out_ref.shape[0]
    part_rows = rows // parts
    members = part_rows * others
    bases = [members * sum(sizes[:h]) for h in range(chunks)]
    groups = local_i // SUB
    deep = local_k // WIDE
    tiles = deep * groups
    pairs = local_k // local_i // 2
    spots = groups * groups
    slabs = part_rows * deep
    slab_tiles = -(-slabs // SUB)
    line = groups * others

    my_row = lax.axis_index("row")
    my_other = lax.axis_index("col") * depths + lax.axis_index("depth")
    me = my_row * others + my_other
    my_part = lax.div(me, members)
    my_slot = lax.rem(me, members)
    part_base = my_part * members

    def device(p):
        q = lax.rem(p, others)
        return (lax.div(p, others), lax.div(q, depths), lax.rem(q, depths))

    loads = [
        pltpu.make_async_copy(far, near, load_sem.at[n])
        for n, (far, near) in enumerate(
            (
                (x_far, x_ref),
                (w_proj_far, w_proj_ref),
                (in_gain_far, in_gain_ref),
                (in_shift_far, in_shift_ref),
                (w_gate_far, w_gate_ref),
                (out_gain_far, out_gain_ref),
                (out_shift_far, out_shift_ref),
                (w_out_far, w_out_ref),
            )
        )
    ]
    for load in loads:
        load.start()
    barrier = pltpu.get_barrier_semaphore()

    def greet(s):
        pl.semaphore_signal(barrier, inc=1, device_id=device(part_base + s), device_id_type=MESH)

    repeat(members - 1, lambda d: greet(lax.rem(my_slot + d + 1, members)))

    loads[1].wait()
    w_turned[...] = w_proj_ref[...].astype(F32).T.astype(BF16)
    for n in (0, 2, 3):
        loads[n].wait()
    values = x_ref[...].astype(F32)
    centred = values - jnp.mean(values, axis=-1, keepdims=True)
    variance = jnp.mean(centred * centred, axis=-1, keepdims=True)
    normed[...] = (
        centred * lax.rsqrt(variance + 1e-05) * in_gain_ref[...].reshape(1, 1, width)
        + in_shift_ref[...].reshape(1, 1, width)
    ).reshape(local_k * local_i, width)

    def edge_block(kg, ig):
        return jnp.concatenate(
            [
                normed[pl.ds(kg * WIDE * local_i + ig * SUB + i, WIDE, stride=local_i), :]
                for i in range(SUB)
            ],
            axis=0,
        ).astype(BF16)

    def gate_block(pair, first, second):
        return jnp.concatenate(
            [
                normed[pl.ds(((2 * pair + b) * local_i + first * SUB + i) * local_i + second * SUB, SUB), :]
                for b in range(2)
                for i in range(SUB)
            ],
            axis=0,
        ).astype(BF16)

    def project(h):
        each = sizes[h]
        part_hidden = members * each
        span1 = each * 2 * tiles
        for t in range(tiles):
            block = edge_block(t // groups, t % groups)
            for side in range(2):
                start = 2 * side * hidden + bases[h]
                gates = dot(w_turned[pl.ds(start, part_hidden), :], block, 1, 1)
                edges = dot(w_turned[pl.ds(start + hidden, part_hidden), :], block, 1, 1)
                packed[pl.ds(side * tiles + t, part_hidden, stride=2 * tiles), :] = (
                    jax.nn.sigmoid(gates) * edges
                )

        def pack(s):
            send1[h][s] = packed[pl.ds(s * span1, span1), :].reshape(send1[h].shape[1:]).astype(BF16)

        repeat(members, pack)

    def exchange(h, n, sent, kept, source, target, p):
        return pltpu.make_async_remote_copy(
            src_ref=sent[h].at[source],
            dst_ref=kept[h].at[target],
            send_sem=sems.at[n, h],
            recv_sem=sems.at[n + 1, h],
            device_id=device(p),
            device_id_type=MESH,
        )

    def copy1(h, s):
        return exchange(h, 0, send1, recv1, s, my_slot, part_base + s)

    def all1(h):
        some = pl.ds(0, members - 1)
        return exchange(h, 0, send1, recv1, some, some, me)

    def copy2(h, p):
        return exchange(h, 2, send2, recv2, p, me, p)

    def all2(h):
        some = pl.ds(0, count - 1)
        return exchange(h, 2, send2, recv2, some, some, me)

    partner = lax.rem(me + count // 2, count)

    def send_off(h):
        project(h)
        if h == 0:
            pl.semaphore_wait(barrier, members - 1 + my_part)

            @pl.when(my_part == 0)
            def _():
                pl.semaphore_signal(barrier, inc=1, device_id=device(partner), device_id_type=MESH)

        repeat(members - 1, lambda d: copy1(h, lax.rem(my_slot + d + 1, members)).start())
        recv1[h][my_slot] = send1[h][my_slot]
        if h == 0:

            @pl.when(my_part == 1)
            def _():
                pl.semaphore_signal(ready, inc=1, device_id=device(partner), device_id_type=MESH)

    for h in range(ahead):
        send_off(h)
    for load in loads[4:]:
        load.wait()
    for t in range(pairs * groups * groups):
        pair, rest = t // (groups * groups), t % (groups * groups)
        gating[t] = jax.nn.sigmoid(
            dot(gate_block(pair, rest // groups, rest % groups), w_gate_ref[...], 1, 0)
        )
    lane = lax.broadcasted_iota(jnp.int32, (line, LANES), 1)
    small_lane = lax.broadcasted_iota(jnp.int32, (SUB, LANES), 1)

    def order(values):
        turned[...] = values
        return jnp.concatenate(
            [
                turned[pl.ds(bases[h] + c, members, stride=sizes[h]), :]
                for h in range(chunks)
                for c in range(sizes[h])
            ],
            axis=0,
        )

    def middle(h):
        each = sizes[h]
        span1 = each * 2 * tiles
        all1(h).wait_recv()

        def take(s):
            gathered[pl.ds(s * span1, span1), :] = recv1[h][s].astype(F32).reshape(span1, LANES)

        repeat(members, take)
        half = SUB * line // 2
        for c in range(each):
            for side in range(2):
                for kt in range(slab_tiles):
                    arrays = []
                    for kb in range(kt * SUB, kt * SUB + SUB):
                        if kb >= slabs:
                            arrays.append(None)
                            continue
                        start = (
                            (kb // deep) * others * span1
                            + (c * 2 + side) * tiles
                            + (kb % deep) * groups
                        )
                        arrays.append(
                            jnp.concatenate(
                                [
                                    gathered[pl.ds(start + g, others, stride=span1), :]
                                    for g in range(groups)
                                ],
                                axis=0,
                            )
                        )
                    turned_blocks = block_transpose(arrays, WIDE, lane)
                    for i in range(SUB):
                        if side == 0:
                            left_rows[kt, pl.ds(i * line, line), :] = turned_blocks[i]
                        else:
                            right_rows[kt, pl.ds(i, line, stride=SUB), :] = turned_blocks[i]
            left = jnp.concatenate(
                [left_rows[kt, pl.ds(b, half, stride=2), :] for b in range(2) for kt in range(slab_tiles)],
                axis=1,
            ).astype(BF16)
            wide = SUB * SUB

            def multiply(j, c=c, left=left):
                right = jnp.concatenate(
                    [right_rows[kt, pl.ds(j * wide, wide), :] for kt in range(slab_tiles)], axis=1
                ).astype(BF16)
                empty = jnp.zeros_like(right)
                both = jnp.concatenate(
                    [jnp.concatenate([right, empty], axis=1), jnp.concatenate([empty, right], axis=1)],
                    axis=0,
                )
                planes[j, pl.ds(c, half, stride=each), :] = dot(left, both, 1, 1)

            repeat(line // SUB, multiply)

        stretch = groups * rows * pairs * each
        unit = pairs * each

        def flatten(j):
            g, q = (j // (others // SUB), j % (others // SUB)) if isinstance(j, int) else (
                lax.div(j, others // SUB),
                lax.rem(j, others // SUB),
            )
            for part in range(stretch // SUB):
                arrays = [planes[j, pl.ds(i * stretch + part * SUB, SUB), :] for i in range(SUB)]
                flat = block_transpose(arrays, SUB, small_lane)
                for n in range(SUB // unit):
                    where = part * (SUB // unit) + n
                    first, r = where // rows, where % rows
                    for o in range(SUB):
                        send2[h][r * others + q * SUB + o, g * groups + first] = flat[o][
                            n * unit : (n + 1) * unit
                        ].astype(BF16)

        repeat(line // SUB, flatten)
        if h == 0:

            @pl.when(my_part == 0)
            def _():
                pl.semaphore_wait(ready, 1)

        repeat(count - 1, lambda d: copy2(h, lax.rem(me + d + 1, count)).start())
        recv2[h][me] = send2[h][me]

    for h in range(chunks):
        middle(h)
        if h + ahead < chunks:
            send_off(h + ahead)
    out_gain = order(jnp.broadcast_to(out_gain_ref[...].reshape(1, hidden), (LANES, hidden)).T)
    out_shift = order(jnp.broadcast_to(out_shift_ref[...].reshape(1, hidden), (LANES, hidden)).T)
    w_out = order(w_out_ref[...].astype(F32)).astype(BF16)
    for h in range(chunks):
        all2(h).wait_recv()
        span2 = spots * pairs * sizes[h]

        def take2(s, h=h, span2=span2):
            total = recv2[h][s].astype(F32)
            for part in range(1, parts):
                total = total + recv2[h][part * members + s].astype(F32)
            start = bases[h] * spots * pairs + s * span2
            gathered2[pl.ds(start, span2), :] = total.reshape(span2, LANES)

        repeat(members, take2)

    for t in range(pairs * groups * groups):
        pair, rest = t // (groups * groups), t % (groups * groups)
        first, second = rest // groups, rest % groups
        spot = (second * groups + first) * pairs + pair
        product = jnp.concatenate(
            [
                gathered2[
                    pl.ds(
                        bases[h] * spots * pairs + spot * sizes[h] + c,
                        members,
                        stride=spots * pairs * sizes[h],
                    ),
                    :,
                ]
                for h in range(chunks)
                for c in range(sizes[h])
            ],
            axis=0,
        )
        spread_out = product - jnp.mean(product, axis=0, keepdims=True)
        moment = jnp.mean(spread_out * spread_out, axis=0, keepdims=True)
        product_norm = (spread_out * lax.rsqrt(moment + 1e-05) * out_gain + out_shift).astype(BF16)
        update = (gating[t] * dot(product_norm, w_out, 0, 0)).astype(BF16)
        for b in range(2):
            out_ref[
                pl.ds((2 * pair + b) * local_i + first * SUB, SUB), pl.ds(second * SUB, SUB), :
            ] = update[b * SUB * SUB : (b + 1) * SUB * SUB].reshape(SUB, SUB, width)

    for h in range(chunks):
        all1(h).wait_send()
        all2(h).wait_send()


def per_device(mesh_sizes, pair_input, in_gain, in_shift, w_proj, w_gate, out_gain, out_shift, w_out):
    rows, cols, depths = mesh_sizes
    parts = 2
    others = cols * depths
    count = rows * others
    local_k, local_i, width = pair_input.shape
    hidden = w_out.shape[0]
    members = count // parts
    own = hidden // members
    sizes = SIZES if sum(SIZES) == own else (own // 2, own // 2)
    groups = local_i // SUB
    tiles = local_k * local_i // LANES
    most = max(sizes)
    line = groups * others
    pairs = local_k // local_i // 2
    spots = groups * groups
    slab_tiles = -(-(rows // parts * local_k) // LANES)
    operands = (
        pair_input,
        w_proj,
        in_gain.reshape(1, -1),
        in_shift.reshape(1, -1),
        w_gate,
        out_gain.reshape(1, -1),
        out_shift.reshape(1, -1),
        w_out,
    )

    def box1(each):
        tall = next(n for n in (SUB, 4, 2, 1) if each * 2 * tiles % n == 0)
        return pltpu.VMEM((members, each * 2 * tiles // tall, tall, LANES), BF16)

    def box2(each):
        return pltpu.VMEM((count, spots, pairs * each, LANES), BF16)

    scratch = [
        *(pltpu.VMEM(a.shape, a.dtype) for a in operands),
        pltpu.SemaphoreType.DMA((len(operands),)),
        pltpu.SemaphoreType.REGULAR,
        pltpu.VMEM((local_k * local_i, width), F32),
        pltpu.VMEM(w_proj.shape[::-1], BF16),
        pltpu.VMEM((tiles, LANES, width), F32),
        pltpu.VMEM((members * most * 2 * tiles, LANES), F32),
        pltpu.VMEM((members * most * 2 * tiles, LANES), F32),
        pltpu.VMEM((slab_tiles, SUB * line, LANES), F32),
        pltpu.VMEM((slab_tiles, SUB * line, LANES), F32),
        pltpu.VMEM((line // SUB, SUB * line // 2 * most, LANES), F32),
        pltpu.VMEM((hidden * spots * pairs, LANES), F32),
        pltpu.VMEM((hidden, LANES), F32),
        pltpu.SemaphoreType.DMA((4, len(sizes))),
        *(box(each) for box in (box1, box1, box2, box2) for each in sizes),
    ]
    return pl.pallas_call(
        functools.partial(kernel, (rows, cols, depths, parts, sizes, min(AHEAD, len(sizes)))),
        out_shape=pltpu.VMEM(pair_input.shape, BF16),
        in_specs=[pl.BlockSpec(memory_space=pltpu.HBM)] * len(operands),
        out_specs=pl.BlockSpec(memory_space=pltpu.VMEM),
        scratch_shapes=scratch,
        compiler_params=pltpu.CompilerParams(
            collective_id=0, has_side_effects=True, vmem_limit_bytes=60_000_000
        ),
    )(*(pltpu.with_memory_space_constraint(a, pltpu.HBM) for a in operands))


def solution(mesh):
    sizes = (mesh.shape["row"], mesh.shape["col"], mesh.shape["depth"])
    placed = (P("row", ("col", "depth"), None), P(), P(), P(), P(), P(), P(), P())
    return jax.shard_map(
        functools.partial(per_device, sizes),
        mesh=mesh,
        in_specs=placed,
        out_specs=P("row", ("col", "depth"), None),
        check_vma=False,
    )
```

```python
import functools

import jax
import jax.numpy as jnp
from jax import lax
from jax.experimental import pallas as pl
from jax.experimental.pallas import tpu as pltpu
from jax.sharding import PartitionSpec as P

F32 = jnp.float32
BF16 = jnp.bfloat16
MESH = pl.DeviceIdType.MESH
LANES = 128
SUB = 8
WIDE = LANES // SUB
UNROLL = 64
SIZES = (2, 2, 4)
AHEAD = 3


def dot(a, b, ca, cb):
    return lax.dot_general(a, b, (((ca,), (cb,)), ((), ())), preferred_element_type=F32)


def repeat(n, body):
    if n <= UNROLL:
        for i in range(n):
            body(i)
    else:
        lax.fori_loop(0, n, lambda i, carry: (body(i), carry)[1], 0)


def choose(mask, x, y):
    if x is None and y is None:
        return None
    return jnp.where(mask, 0.0 if x is None else x, 0.0 if y is None else y)


def gather_blocks(arrays, block, lane):
    arrays = [arrays[-q % SUB] for q in range(SUB)]
    for d in (1, 2, 4):
        moved = (lane // block) & d != 0
        arrays = [choose(moved, arrays[(q - d) % SUB], arrays[q]) for q in range(SUB)]
    return arrays


def kernel(
    plan,
    x_far,
    w_proj_far,
    in_gain_far,
    in_shift_far,
    w_gate_far,
    out_gain_far,
    out_shift_far,
    w_out_far,
    out_ref,
    x_ref,
    w_proj_ref,
    in_gain_ref,
    in_shift_ref,
    w_gate_ref,
    out_gain_ref,
    out_shift_ref,
    w_out_ref,
    load_sem,
    ready,
    normed,
    w_turned,
    blocks,
    gating,
    packed,
    gathered,
    left_rows,
    right_rows,
    planes,
    gathered2,
    turned,
    sems,
    *boxes,
):
    rows, cols, depths, parts, sizes, ahead = plan
    chunks = len(sizes)
    send1, recv1, send2, recv2 = (boxes[n * chunks : (n + 1) * chunks] for n in range(4))
    others = cols * depths
    count = rows * others
    local_k, local_i, width = x_ref.shape
    hidden = w_out_ref.shape[0]
    part_rows = rows // parts
    members = part_rows * others
    bases = [members * sum(sizes[:h]) for h in range(chunks)]
    groups = local_i // SUB
    deep = local_k // WIDE
    tiles = deep * groups
    pairs = local_k // local_i // 2
    spots = groups * groups
    slabs = part_rows * deep
    slab_tiles = -(-slabs // SUB)
    line = groups * others

    my_row = lax.axis_index("row")
    my_other = lax.axis_index("col") * depths + lax.axis_index("depth")
    me = my_row * others + my_other
    my_part = lax.div(me, members)
    my_slot = lax.rem(me, members)
    part_base = my_part * members

    def device(p):
        q = lax.rem(p, others)
        return (lax.div(p, others), lax.div(q, depths), lax.rem(q, depths))

    loads = [
        pltpu.make_async_copy(far, near, load_sem.at[n])
        for n, (far, near) in enumerate(
            (
                (x_far, x_ref),
                (w_proj_far, w_proj_ref),
                (in_gain_far, in_gain_ref),
                (in_shift_far, in_shift_ref),
                (w_gate_far, w_gate_ref),
                (out_gain_far, out_gain_ref),
                (out_shift_far, out_shift_ref),
                (w_out_far, w_out_ref),
            )
        )
    ]
    for load in loads:
        load.start()
    barrier = pltpu.get_barrier_semaphore()

    def greet(s):
        pl.semaphore_signal(barrier, inc=1, device_id=device(part_base + s), device_id_type=MESH)

    repeat(members - 1, lambda d: greet(lax.rem(my_slot + d + 1, members)))

    loads[1].wait()
    w_flat = w_proj_ref[...].astype(F32).T.astype(BF16)
    for h in range(chunks):
        size = members * sizes[h]
        for n in range(4):
            w_turned[pl.ds(4 * bases[h] + n * size, size), :] = w_flat[
                n * hidden + bases[h] : n * hidden + bases[h] + size
            ]
    for n in (0, 2, 3):
        loads[n].wait()
    values = x_ref[...].astype(F32)
    centred = values - jnp.mean(values, axis=-1, keepdims=True)
    variance = jnp.mean(centred * centred, axis=-1, keepdims=True)
    normed[...] = (
        centred * lax.rsqrt(variance + 1e-05) * in_gain_ref[...].reshape(1, 1, width)
        + in_shift_ref[...].reshape(1, 1, width)
    ).reshape(local_k * local_i, width)

    first_slab = lax.rem(my_row, part_rows) * deep
    my_turn = lax.rem(my_other, SUB)

    def edge_block(kg, ig):
        return jnp.concatenate(
            [
                normed[
                    pl.ds(
                        kg * WIDE * local_i
                        + ig * SUB
                        + lax.rem(p + SUB * part_rows * deep - first_slab - kg, SUB),
                        WIDE,
                        stride=local_i,
                    ),
                    :,
                ]
                for p in range(SUB)
            ],
            axis=0,
        ).astype(BF16)

    def place(pair, first, p):
        i = lax.rem(p + 2 * SUB - my_turn, 2 * SUB)
        return (2 * pair + lax.div(i, SUB)) * local_i + first * SUB + lax.rem(i, SUB)

    def gate_block(pair, first, second):
        return jnp.concatenate(
            [
                normed[pl.ds(pl.multiple_of(place(pair, first, p) * local_i + second * SUB, SUB), SUB), :]
                for p in range(2 * SUB)
            ],
            axis=0,
        ).astype(BF16)

    def project(h):
        each = sizes[h]
        part_hidden = members * each
        span1 = each * 2 * tiles
        for t in range(tiles):
            if h == 0:
                blocks[t] = edge_block(t // groups, t % groups)
            projected = dot(w_turned[pl.ds(4 * bases[h], 4 * part_hidden), :], blocks[t], 1, 1)
            for side in range(2):
                gates = projected[2 * side * part_hidden : (2 * side + 1) * part_hidden]
                edges = projected[(2 * side + 1) * part_hidden : (2 * side + 2) * part_hidden]
                packed[pl.ds(side * tiles + t, part_hidden, stride=2 * tiles), :] = (
                    jax.nn.sigmoid(gates) * edges
                )

        def pack(s):
            send1[h][s] = packed[pl.ds(s * span1, span1), :].reshape(send1[h].shape[1:]).astype(BF16)

        repeat(members, pack)

    def exchange(h, n, sent, kept, source, target, p):
        return pltpu.make_async_remote_copy(
            src_ref=sent[h].at[source],
            dst_ref=kept[h].at[target],
            send_sem=sems.at[n, h],
            recv_sem=sems.at[n + 1, h],
            device_id=device(p),
            device_id_type=MESH,
        )

    def copy1(h, s):
        return exchange(h, 0, send1, recv1, s, my_slot, part_base + s)

    def all1(h):
        some = pl.ds(0, members - 1)
        return exchange(h, 0, send1, recv1, some, some, me)

    def copy2(h, p):
        return exchange(h, 2, send2, recv2, p, me, p)

    def all2(h):
        some = pl.ds(0, count - 1)
        return exchange(h, 2, send2, recv2, some, some, me)

    partner = lax.rem(me + count // 2, count)

    def send_off(h):
        project(h)
        if h == 0:
            pl.semaphore_wait(barrier, members - 1 + my_part)

            @pl.when(my_part == 0)
            def _():
                pl.semaphore_signal(barrier, inc=1, device_id=device(partner), device_id_type=MESH)

        repeat(members - 1, lambda d: copy1(h, lax.rem(my_slot + d + 1, members)).start())
        recv1[h][my_slot] = send1[h][my_slot]
        if h == 0:

            @pl.when(my_part == 1)
            def _():
                pl.semaphore_signal(ready, inc=1, device_id=device(partner), device_id_type=MESH)

    for h in range(ahead):
        send_off(h)
    for load in loads[4:]:
        load.wait()
    for t in range(pairs * groups * groups):
        pair, rest = t // (groups * groups), t % (groups * groups)
        gating[t] = jax.nn.sigmoid(
            dot(gate_block(pair, rest // groups, rest % groups), w_gate_ref[...], 1, 0)
        )
    lane = lax.broadcasted_iota(jnp.int32, (line, LANES), 1)
    small_lane = lax.broadcasted_iota(jnp.int32, (SUB, LANES), 1)

    def order(values):
        turned[...] = values
        return jnp.concatenate(
            [
                turned[pl.ds(bases[h] + c, members, stride=sizes[h]), :]
                for h in range(chunks)
                for c in range(sizes[h])
            ],
            axis=0,
        )

    def middle(h):
        each = sizes[h]
        span1 = each * 2 * tiles
        all1(h).wait_recv()

        def take(s):
            gathered[pl.ds(s * span1, span1), :] = recv1[h][s].astype(F32).reshape(span1, LANES)

        repeat(members, take)
        half = SUB * line // 2
        for c in range(each):
            for side in range(2):
                for kt in range(slab_tiles):
                    arrays = []
                    for kb in range(kt * SUB, kt * SUB + SUB):
                        if kb >= slabs:
                            arrays.append(None)
                            continue
                        start = (
                            (kb // deep) * others * span1
                            + (c * 2 + side) * tiles
                            + (kb % deep) * groups
                        )
                        arrays.append(
                            jnp.concatenate(
                                [
                                    gathered[pl.ds(start + g, others, stride=span1), :]
                                    for g in range(groups)
                                ],
                                axis=0,
                            )
                        )
                    for i, found in enumerate(gather_blocks(arrays, WIDE, lane)):
                        turned_back = pltpu.roll(found, LANES - i * WIDE, 1) if i else found
                        if side == 0:
                            left_rows[kt, pl.ds(i * line, line), :] = turned_back
                        else:
                            right_rows[kt, pl.ds(i, line, stride=SUB), :] = turned_back
            left = jnp.concatenate(
                [left_rows[kt, pl.ds(b, half, stride=2), :] for b in range(2) for kt in range(slab_tiles)],
                axis=1,
            ).astype(BF16)
            wide = SUB * SUB

            def multiply(j, c=c, left=left):
                right = jnp.concatenate(
                    [right_rows[kt, pl.ds(j * wide, wide), :] for kt in range(slab_tiles)], axis=1
                ).astype(BF16)
                empty = jnp.zeros_like(right)
                both = jnp.concatenate(
                    [jnp.concatenate([right, empty], axis=1), jnp.concatenate([empty, right], axis=1)],
                    axis=0,
                )
                planes[j, pl.ds(c, half, stride=each), :] = dot(left, both, 1, 1)

            repeat(line // SUB, multiply)

        stretch = groups * rows * pairs * each
        unit = pairs * each

        def flatten(j):
            g, q = (j // (others // SUB), j % (others // SUB)) if isinstance(j, int) else (
                lax.div(j, others // SUB),
                lax.rem(j, others // SUB),
            )
            for part in range(stretch // SUB):
                arrays = [planes[j, pl.ds(i * stretch + part * SUB, SUB), :] for i in range(SUB)]
                arrays = [pltpu.roll(a, i * SUB, 1) if i else a for i, a in enumerate(arrays)]
                flat = gather_blocks(arrays, SUB, small_lane)
                for n in range(SUB // unit):
                    where = part * (SUB // unit) + n
                    first, r = where // rows, where % rows
                    for o in range(SUB):
                        send2[h][r * others + q * SUB + o, g * groups + first] = flat[o][
                            n * unit : (n + 1) * unit
                        ].astype(BF16)

        repeat(line // SUB, flatten)
        if h == 0:

            @pl.when(my_part == 0)
            def _():
                pl.semaphore_wait(ready, 1)

        repeat(count - 1, lambda d: copy2(h, lax.rem(me + d + 1, count)).start())
        recv2[h][me] = send2[h][me]

    for h in range(chunks):
        middle(h)
        if h + ahead < chunks:
            send_off(h + ahead)
    out_gain = order(jnp.broadcast_to(out_gain_ref[...].reshape(1, hidden), (LANES, hidden)).T)
    out_shift = order(jnp.broadcast_to(out_shift_ref[...].reshape(1, hidden), (LANES, hidden)).T)
    w_out = order(w_out_ref[...].astype(F32)).astype(BF16)
    for h in range(chunks):
        all2(h).wait_recv()
        span2 = spots * pairs * sizes[h]

        def take2(s, h=h, span2=span2):
            total = recv2[h][s].astype(F32)
            for part in range(1, parts):
                total = total + recv2[h][part * members + s].astype(F32)
            start = bases[h] * spots * pairs + s * span2
            gathered2[pl.ds(start, span2), :] = total.reshape(span2, LANES)

        repeat(members, take2)

    for t in range(pairs * groups * groups):
        pair, rest = t // (groups * groups), t % (groups * groups)
        first, second = rest // groups, rest % groups
        spot = (second * groups + first) * pairs + pair
        product = jnp.concatenate(
            [
                gathered2[
                    pl.ds(
                        bases[h] * spots * pairs + spot * sizes[h] + c,
                        members,
                        stride=spots * pairs * sizes[h],
                    ),
                    :,
                ]
                for h in range(chunks)
                for c in range(sizes[h])
            ],
            axis=0,
        )
        spread_out = product - jnp.mean(product, axis=0, keepdims=True)
        moment = jnp.mean(spread_out * spread_out, axis=0, keepdims=True)
        product_norm = (spread_out * lax.rsqrt(moment + 1e-05) * out_gain + out_shift).astype(BF16)
        update = (gating[t] * dot(product_norm, w_out, 0, 0)).astype(BF16)
        for p in range(2 * SUB):
            out_ref[place(pair, first, p), pl.ds(second * SUB, SUB), :] = update[p * SUB : (p + 1) * SUB]

    for h in range(chunks):
        all1(h).wait_send()
        all2(h).wait_send()


def per_device(mesh_sizes, pair_input, in_gain, in_shift, w_proj, w_gate, out_gain, out_shift, w_out):
    rows, cols, depths = mesh_sizes
    parts = 2
    others = cols * depths
    count = rows * others
    local_k, local_i, width = pair_input.shape
    hidden = w_out.shape[0]
    members = count // parts
    own = hidden // members
    sizes = SIZES if sum(SIZES) == own else (own // 2, own // 2)
    groups = local_i // SUB
    tiles = local_k * local_i // LANES
    most = max(sizes)
    line = groups * others
    pairs = local_k // local_i // 2
    spots = groups * groups
    slab_tiles = -(-(rows // parts * local_k) // LANES)
    operands = (
        pair_input,
        w_proj,
        in_gain.reshape(1, -1),
        in_shift.reshape(1, -1),
        w_gate,
        out_gain.reshape(1, -1),
        out_shift.reshape(1, -1),
        w_out,
    )

    def box1(each):
        tall = next(n for n in (SUB, 4, 2, 1) if each * 2 * tiles % n == 0)
        return pltpu.VMEM((members, each * 2 * tiles // tall, tall, LANES), BF16)

    def box2(each):
        return pltpu.VMEM((count, spots, pairs * each, LANES), BF16)

    scratch = [
        *(pltpu.VMEM(a.shape, a.dtype) for a in operands),
        pltpu.SemaphoreType.DMA((len(operands),)),
        pltpu.SemaphoreType.REGULAR,
        pltpu.VMEM((local_k * local_i, width), F32),
        pltpu.VMEM(w_proj.shape[::-1], BF16),
        pltpu.VMEM((tiles, LANES, width), BF16),
        pltpu.VMEM((tiles, LANES, width), F32),
        pltpu.VMEM((members * most * 2 * tiles, LANES), F32),
        pltpu.VMEM((members * most * 2 * tiles, LANES), F32),
        pltpu.VMEM((slab_tiles, SUB * line, LANES), F32),
        pltpu.VMEM((slab_tiles, SUB * line, LANES), F32),
        pltpu.VMEM((line // SUB, SUB * line // 2 * most, LANES), F32),
        pltpu.VMEM((hidden * spots * pairs, LANES), F32),
        pltpu.VMEM((hidden, LANES), F32),
        pltpu.SemaphoreType.DMA((4, len(sizes))),
        *(box(each) for box in (box1, box1, box2, box2) for each in sizes),
    ]
    return pl.pallas_call(
        functools.partial(kernel, (rows, cols, depths, parts, sizes, min(AHEAD, len(sizes)))),
        out_shape=pltpu.VMEM(pair_input.shape, BF16),
        in_specs=[pl.BlockSpec(memory_space=pltpu.HBM)] * len(operands),
        out_specs=pl.BlockSpec(memory_space=pltpu.VMEM),
        scratch_shapes=scratch,
        compiler_params=pltpu.CompilerParams(
            collective_id=0, has_side_effects=True, vmem_limit_bytes=60_000_000
        ),
    )(*(pltpu.with_memory_space_constraint(a, pltpu.HBM) for a in operands))


def solution(mesh):
    sizes = (mesh.shape["row"], mesh.shape["col"], mesh.shape["depth"])
    placed = (P("row", ("col", "depth"), None), P(), P(), P(), P(), P(), P(), P())
    return jax.shard_map(
        functools.partial(per_device, sizes),
        mesh=mesh,
        in_specs=placed,
        out_specs=P("row", ("col", "depth"), None),
        check_vma=False,
    )
```

```python
import functools

import jax
import jax.numpy as jnp
from jax import lax
from jax.experimental import pallas as pl
from jax.experimental.pallas import tpu as pltpu
from jax.sharding import PartitionSpec as P

F32 = jnp.float32
BF16 = jnp.bfloat16
MESH = pl.DeviceIdType.MESH
LANES = 128
SUB = 8
WIDE = LANES // SUB
UNROLL = 64
SIZES = (2, 2, 4)
AHEAD = 3


def dot(a, b, ca, cb):
    return lax.dot_general(a, b, (((ca,), (cb,)), ((), ())), preferred_element_type=F32)


def repeat(n, body):
    if n <= UNROLL:
        for i in range(n):
            body(i)
    else:
        lax.fori_loop(0, n, lambda i, carry: (body(i), carry)[1], 0)


def choose(mask, x, y):
    if x is None and y is None:
        return None
    return jnp.where(mask, 0.0 if x is None else x, 0.0 if y is None else y)


def gather_blocks(arrays, block, lane):
    arrays = [arrays[-q % SUB] for q in range(SUB)]
    for d in (1, 2, 4):
        moved = (lane // block) & d != 0
        arrays = [choose(moved, arrays[(q - d) % SUB], arrays[q]) for q in range(SUB)]
    return arrays


def kernel(
    plan,
    x_far,
    w_proj_far,
    in_gain_far,
    in_shift_far,
    w_gate_far,
    out_gain_far,
    out_shift_far,
    w_out_far,
    out_ref,
    x_ref,
    w_proj_ref,
    in_gain_ref,
    in_shift_ref,
    w_gate_ref,
    out_gain_ref,
    out_shift_ref,
    w_out_ref,
    load_sem,
    ready,
    normed,
    w_turned,
    blocks,
    gating,
    packed,
    gathered,
    left_rows,
    right_rows,
    planes,
    gathered2,
    turned,
    sems,
    *boxes,
):
    rows, cols, depths, parts, sizes, ahead = plan
    chunks = len(sizes)
    send1, recv1, send2, recv2 = (boxes[n * chunks : (n + 1) * chunks] for n in range(4))
    others = cols * depths
    count = rows * others
    local_k, local_i, width = x_ref.shape
    hidden = w_out_ref.shape[0]
    part_rows = rows // parts
    members = part_rows * others
    bases = [members * sum(sizes[:h]) for h in range(chunks)]
    groups = local_i // SUB
    deep = local_k // WIDE
    tiles = deep * groups
    pairs = local_k // local_i // 2
    spots = groups * groups
    slabs = part_rows * deep
    slab_tiles = -(-slabs // SUB)
    line = groups * others

    my_row = lax.axis_index("row")
    my_other = lax.axis_index("col") * depths + lax.axis_index("depth")
    me = my_row * others + my_other
    my_part = lax.div(me, members)
    my_slot = lax.rem(me, members)
    part_base = my_part * members

    def device(p):
        q = lax.rem(p, others)
        return (lax.div(p, others), lax.div(q, depths), lax.rem(q, depths))

    loads = [
        pltpu.make_async_copy(far, near, load_sem.at[n])
        for n, (far, near) in enumerate(
            (
                (x_far, x_ref),
                (w_proj_far, w_proj_ref),
                (in_gain_far, in_gain_ref),
                (in_shift_far, in_shift_ref),
                (w_gate_far, w_gate_ref),
                (out_gain_far, out_gain_ref),
                (out_shift_far, out_shift_ref),
                (w_out_far, w_out_ref),
            )
        )
    ]
    for load in loads:
        load.start()
    barrier = pltpu.get_barrier_semaphore()

    def greet(s):
        pl.semaphore_signal(barrier, inc=1, device_id=device(part_base + s), device_id_type=MESH)

    repeat(members - 1, lambda d: greet(lax.rem(my_slot + d + 1, members)))

    loads[1].wait()
    w_flat = w_proj_ref[...].astype(F32).T.astype(BF16)
    for h in range(chunks):
        size = members * sizes[h]
        for n in range(4):
            w_turned[pl.ds(4 * bases[h] + n * size, size), :] = w_flat[
                n * hidden + bases[h] : n * hidden + bases[h] + size
            ]
    for n in (0, 2, 3):
        loads[n].wait()
    values = x_ref[...].astype(F32)
    centred = values - jnp.mean(values, axis=-1, keepdims=True)
    variance = jnp.mean(centred * centred, axis=-1, keepdims=True)
    normed[...] = (
        centred * lax.rsqrt(variance + 1e-05) * in_gain_ref[...].reshape(1, 1, width)
        + in_shift_ref[...].reshape(1, 1, width)
    ).reshape(local_k * local_i, width)

    first_slab = lax.rem(my_row, part_rows) * deep
    my_turn = lax.rem(my_other, SUB)

    def edge_block(kg, ig):
        return jnp.concatenate(
            [
                normed[
                    pl.ds(
                        kg * WIDE * local_i
                        + ig * SUB
                        + lax.rem(p + SUB * part_rows * deep - first_slab - kg, SUB),
                        WIDE,
                        stride=local_i,
                    ),
                    :,
                ]
                for p in range(SUB)
            ],
            axis=0,
        ).astype(BF16)

    def place(pair, first, p):
        i = lax.rem(p + 2 * SUB - my_turn, 2 * SUB)
        return (2 * pair + lax.div(i, SUB)) * local_i + first * SUB + lax.rem(i, SUB)

    def gate_block(pair, first, second):
        return jnp.concatenate(
            [
                normed[pl.ds(pl.multiple_of(place(pair, first, p) * local_i + second * SUB, SUB), SUB), :]
                for p in range(2 * SUB)
            ],
            axis=0,
        ).astype(BF16)

    def project(h):
        each = sizes[h]
        part_hidden = members * each
        span1 = each * 2 * tiles
        for t in range(tiles):
            if h == 0:
                blocks[t] = edge_block(t // groups, t % groups)
            projected = dot(w_turned[pl.ds(4 * bases[h], 4 * part_hidden), :], blocks[t], 1, 1)
            for side in range(2):
                gates = projected[2 * side * part_hidden : (2 * side + 1) * part_hidden]
                edges = projected[(2 * side + 1) * part_hidden : (2 * side + 2) * part_hidden]
                packed[pl.ds(side * tiles + t, part_hidden, stride=2 * tiles), :] = (
                    jax.nn.sigmoid(gates) * edges
                )

        def pack(s):
            send1[h][s] = packed[pl.ds(s * span1, span1), :].reshape(send1[h].shape[1:]).astype(BF16)

        repeat(members, pack)

    def exchange(h, n, sent, kept, source, target, p):
        return pltpu.make_async_remote_copy(
            src_ref=sent[h].at[source],
            dst_ref=kept[h].at[target],
            send_sem=sems.at[n, h],
            recv_sem=sems.at[n + 1, h],
            device_id=device(p),
            device_id_type=MESH,
        )

    def copy1(h, s):
        return exchange(h, 0, send1, recv1, s, my_slot, part_base + s)

    def all1(h):
        some = pl.ds(0, members - 1)
        return exchange(h, 0, send1, recv1, some, some, me)

    def copy2(h, p):
        return exchange(h, 2, send2, recv2, p, me, p)

    def all2(h):
        some = pl.ds(0, count - 1)
        return exchange(h, 2, send2, recv2, some, some, me)

    def stop(k):
        other = jnp.where(k > my_row, k, k - 1)
        return jnp.where((k == 0) | (k == rows), my_row, other)

    def route(d):
        k, e = (d + 1) // others, (d + 1) % others
        row = jnp.where(my_other + e >= others, stop(k + 1), stop(k))
        return row * others + lax.rem(my_other + e, others)

    routes = [route(d) for d in range(count - 1 if count <= UNROLL else 0)]
    partner = lax.rem(me + count // 2, count)

    def send_off(h):
        project(h)
        if h == 0:
            pl.semaphore_wait(barrier, members - 1 + my_part)

            @pl.when(my_part == 0)
            def _():
                pl.semaphore_signal(barrier, inc=1, device_id=device(partner), device_id_type=MESH)

        repeat(members - 1, lambda d: copy1(h, lax.rem(my_slot + members - 1 - d, members)).start())
        recv1[h][my_slot] = send1[h][my_slot]
        if h == 0:

            @pl.when(my_part == 1)
            def _():
                pl.semaphore_signal(ready, inc=1, device_id=device(partner), device_id_type=MESH)

    for h in range(ahead):
        send_off(h)
    for load in loads[4:]:
        load.wait()
    for t in range(pairs * groups * groups):
        pair, rest = t // (groups * groups), t % (groups * groups)
        gating[t] = jax.nn.sigmoid(
            dot(gate_block(pair, rest // groups, rest % groups), w_gate_ref[...], 1, 0)
        )
    lane = lax.broadcasted_iota(jnp.int32, (line, LANES), 1)
    small_lane = lax.broadcasted_iota(jnp.int32, (SUB, LANES), 1)

    def order(values):
        turned[...] = values
        return jnp.concatenate(
            [
                turned[pl.ds(bases[h] + c, members, stride=sizes[h]), :]
                for h in range(chunks)
                for c in range(sizes[h])
            ],
            axis=0,
        )

    def middle(h):
        each = sizes[h]
        span1 = each * 2 * tiles
        all1(h).wait_recv()

        def take(s):
            gathered[pl.ds(s * span1, span1), :] = recv1[h][s].astype(F32).reshape(span1, LANES)

        repeat(members, take)
        half = SUB * line // 2
        for c in range(each):
            for side in range(2):
                for kt in range(slab_tiles):
                    arrays = []
                    for kb in range(kt * SUB, kt * SUB + SUB):
                        if kb >= slabs:
                            arrays.append(None)
                            continue
                        start = (
                            (kb // deep) * others * span1
                            + (c * 2 + side) * tiles
                            + (kb % deep) * groups
                        )
                        arrays.append(
                            jnp.concatenate(
                                [
                                    gathered[pl.ds(start + g, others, stride=span1), :]
                                    for g in range(groups)
                                ],
                                axis=0,
                            )
                        )
                    for i, found in enumerate(gather_blocks(arrays, WIDE, lane)):
                        turned_back = pltpu.roll(found, LANES - i * WIDE, 1) if i else found
                        if side == 0:
                            left_rows[kt, pl.ds(i * line, line), :] = turned_back
                        else:
                            right_rows[kt, pl.ds(i, line, stride=SUB), :] = turned_back
            left = jnp.concatenate(
                [left_rows[kt, pl.ds(b, half, stride=2), :] for b in range(2) for kt in range(slab_tiles)],
                axis=1,
            ).astype(BF16)
            wide = SUB * SUB

            def multiply(j, c=c, left=left):
                right = jnp.concatenate(
                    [right_rows[kt, pl.ds(j * wide, wide), :] for kt in range(slab_tiles)], axis=1
                ).astype(BF16)
                empty = jnp.zeros_like(right)
                both = jnp.concatenate(
                    [jnp.concatenate([right, empty], axis=1), jnp.concatenate([empty, right], axis=1)],
                    axis=0,
                )
                planes[j, pl.ds(c, half, stride=each), :] = dot(left, both, 1, 1)

            repeat(line // SUB, multiply)

        stretch = groups * rows * pairs * each
        unit = pairs * each

        def flatten(j):
            g, q = (j // (others // SUB), j % (others // SUB)) if isinstance(j, int) else (
                lax.div(j, others // SUB),
                lax.rem(j, others // SUB),
            )
            for part in range(stretch // SUB):
                arrays = [planes[j, pl.ds(i * stretch + part * SUB, SUB), :] for i in range(SUB)]
                arrays = [pltpu.roll(a, i * SUB, 1) if i else a for i, a in enumerate(arrays)]
                flat = gather_blocks(arrays, SUB, small_lane)
                for n in range(SUB // unit):
                    where = part * (SUB // unit) + n
                    first, r = where // rows, where % rows
                    for o in range(SUB):
                        send2[h][r * others + q * SUB + o, g * groups + first] = flat[o][
                            n * unit : (n + 1) * unit
                        ].astype(BF16)

        repeat(line // SUB, flatten)
        if h == 0:

            @pl.when(my_part == 0)
            def _():
                pl.semaphore_wait(ready, 1)

        repeat(count - 1, lambda d: copy2(h, routes[d] if isinstance(d, int) else route(d)).start())
        recv2[h][me] = send2[h][me]

    for h in range(chunks):
        middle(h)
        if h + ahead < chunks:
            send_off(h + ahead)
    out_gain = order(jnp.broadcast_to(out_gain_ref[...].reshape(1, hidden), (LANES, hidden)).T)
    out_shift = order(jnp.broadcast_to(out_shift_ref[...].reshape(1, hidden), (LANES, hidden)).T)
    w_out = order(w_out_ref[...].astype(F32)).astype(BF16)
    for h in range(chunks):
        all2(h).wait_recv()
        span2 = spots * pairs * sizes[h]

        def take2(s, h=h, span2=span2):
            total = recv2[h][s].astype(F32)
            for part in range(1, parts):
                total = total + recv2[h][part * members + s].astype(F32)
            start = bases[h] * spots * pairs + s * span2
            gathered2[pl.ds(start, span2), :] = total.reshape(span2, LANES)

        repeat(members, take2)

    for t in range(pairs * groups * groups):
        pair, rest = t // (groups * groups), t % (groups * groups)
        first, second = rest // groups, rest % groups
        spot = (second * groups + first) * pairs + pair
        product = jnp.concatenate(
            [
                gathered2[
                    pl.ds(
                        bases[h] * spots * pairs + spot * sizes[h] + c,
                        members,
                        stride=spots * pairs * sizes[h],
                    ),
                    :,
                ]
                for h in range(chunks)
                for c in range(sizes[h])
            ],
            axis=0,
        )
        spread_out = product - jnp.mean(product, axis=0, keepdims=True)
        moment = jnp.mean(spread_out * spread_out, axis=0, keepdims=True)
        product_norm = (spread_out * lax.rsqrt(moment + 1e-05) * out_gain + out_shift).astype(BF16)
        update = (gating[t] * dot(product_norm, w_out, 0, 0)).astype(BF16)
        for p in range(2 * SUB):
            out_ref[place(pair, first, p), pl.ds(second * SUB, SUB), :] = update[p * SUB : (p + 1) * SUB]

    for h in range(chunks):
        all1(h).wait_send()
        all2(h).wait_send()


def per_device(mesh_sizes, pair_input, in_gain, in_shift, w_proj, w_gate, out_gain, out_shift, w_out):
    rows, cols, depths = mesh_sizes
    parts = 2
    others = cols * depths
    count = rows * others
    local_k, local_i, width = pair_input.shape
    hidden = w_out.shape[0]
    members = count // parts
    own = hidden // members
    sizes = SIZES if sum(SIZES) == own else (own // 2, own // 2)
    groups = local_i // SUB
    tiles = local_k * local_i // LANES
    most = max(sizes)
    line = groups * others
    pairs = local_k // local_i // 2
    spots = groups * groups
    slab_tiles = -(-(rows // parts * local_k) // LANES)
    operands = (
        pair_input,
        w_proj,
        in_gain.reshape(1, -1),
        in_shift.reshape(1, -1),
        w_gate,
        out_gain.reshape(1, -1),
        out_shift.reshape(1, -1),
        w_out,
    )

    def box1(each):
        tall = next(n for n in (SUB, 4, 2, 1) if each * 2 * tiles % n == 0)
        return pltpu.VMEM((members, each * 2 * tiles // tall, tall, LANES), BF16)

    def box2(each):
        return pltpu.VMEM((count, spots, pairs * each, LANES), BF16)

    scratch = [
        *(pltpu.VMEM(a.shape, a.dtype) for a in operands),
        pltpu.SemaphoreType.DMA((len(operands),)),
        pltpu.SemaphoreType.REGULAR,
        pltpu.VMEM((local_k * local_i, width), F32),
        pltpu.VMEM(w_proj.shape[::-1], BF16),
        pltpu.VMEM((tiles, LANES, width), BF16),
        pltpu.VMEM((tiles, LANES, width), F32),
        pltpu.VMEM((members * most * 2 * tiles, LANES), F32),
        pltpu.VMEM((members * most * 2 * tiles, LANES), F32),
        pltpu.VMEM((slab_tiles, SUB * line, LANES), F32),
        pltpu.VMEM((slab_tiles, SUB * line, LANES), F32),
        pltpu.VMEM((line // SUB, SUB * line // 2 * most, LANES), F32),
        pltpu.VMEM((hidden * spots * pairs, LANES), F32),
        pltpu.VMEM((hidden, LANES), F32),
        pltpu.SemaphoreType.DMA((4, len(sizes))),
        *(box(each) for box in (box1, box1, box2, box2) for each in sizes),
    ]
    return pl.pallas_call(
        functools.partial(kernel, (rows, cols, depths, parts, sizes, min(AHEAD, len(sizes)))),
        out_shape=pltpu.VMEM(pair_input.shape, BF16),
        in_specs=[pl.BlockSpec(memory_space=pltpu.HBM)] * len(operands),
        out_specs=pl.BlockSpec(memory_space=pltpu.VMEM),
        scratch_shapes=scratch,
        compiler_params=pltpu.CompilerParams(
            collective_id=0, has_side_effects=True, vmem_limit_bytes=60_000_000
        ),
    )(*(pltpu.with_memory_space_constraint(a, pltpu.HBM) for a in operands))


def solution(mesh):
    sizes = (mesh.shape["row"], mesh.shape["col"], mesh.shape["depth"])
    placed = (P("row", ("col", "depth"), None), P(), P(), P(), P(), P(), P(), P())
    return jax.shard_map(
        functools.partial(per_device, sizes),
        mesh=mesh,
        in_specs=placed,
        out_specs=P("row", ("col", "depth"), None),
        check_vma=False,
    )
```

```python
import functools

import jax
import jax.numpy as jnp
from jax import lax
from jax.experimental import pallas as pl
from jax.experimental.pallas import tpu as pltpu
from jax.sharding import PartitionSpec as P

F32 = jnp.float32
BF16 = jnp.bfloat16
MESH = pl.DeviceIdType.MESH
LANES = 128
SUB = 8
WIDE = LANES // SUB
UNROLL = 64
SIZES = (2, 2, 4)
AHEAD = 3


def dot(a, b, ca, cb):
    return lax.dot_general(a, b, (((ca,), (cb,)), ((), ())), preferred_element_type=F32)


def repeat(n, body):
    if n <= UNROLL:
        for i in range(n):
            body(i)
    else:
        lax.fori_loop(0, n, lambda i, carry: (body(i), carry)[1], 0)


def choose(mask, x, y):
    if x is None and y is None:
        return None
    return jnp.where(mask, 0.0 if x is None else x, 0.0 if y is None else y)


def gather_blocks(arrays, block, lane):
    arrays = [arrays[-q % SUB] for q in range(SUB)]
    for d in (1, 2, 4):
        moved = (lane // block) & d != 0
        arrays = [choose(moved, arrays[(q - d) % SUB], arrays[q]) for q in range(SUB)]
    return arrays


def kernel(
    plan,
    x_far,
    w_proj_far,
    in_gain_far,
    in_shift_far,
    w_gate_far,
    out_gain_far,
    out_shift_far,
    w_out_far,
    out_ref,
    x_ref,
    w_proj_ref,
    in_gain_ref,
    in_shift_ref,
    w_gate_ref,
    out_gain_ref,
    out_shift_ref,
    w_out_ref,
    load_sem,
    ready,
    normed,
    w_turned,
    blocks,
    gating,
    packed,
    gathered,
    left_rows,
    right_rows,
    planes,
    gathered2,
    turned,
    sems,
    *boxes,
):
    rows, cols, depths, parts, sizes, ahead = plan
    chunks = len(sizes)
    send1, recv1, send2, recv2 = (boxes[n * chunks : (n + 1) * chunks] for n in range(4))
    slabs_near = boxes[4 * chunks :]
    others = cols * depths
    count = rows * others
    local_k, local_i, width = x_ref.shape
    hidden = w_out_ref.shape[0]
    part_rows = rows // parts
    members = part_rows * others
    bases = [members * sum(sizes[:h]) for h in range(chunks)]
    groups = local_i // SUB
    deep = local_k // WIDE
    tiles = deep * groups
    pairs = local_k // local_i // 2
    spots = groups * groups
    slabs = part_rows * deep
    slab_tiles = -(-slabs // SUB)
    line = groups * others

    my_row = lax.axis_index("row")
    my_other = lax.axis_index("col") * depths + lax.axis_index("depth")
    me = my_row * others + my_other
    my_part = lax.div(me, members)
    my_slot = lax.rem(me, members)
    part_base = my_part * members

    def device(p):
        q = lax.rem(p, others)
        return (lax.div(p, others), lax.div(q, depths), lax.rem(q, depths))

    loads = [
        pltpu.make_async_copy(far, near, load_sem.at[n])
        for n, (far, near) in enumerate(
            (
                (x_far, x_ref),
                (w_proj_far, w_proj_ref),
                (in_gain_far, in_gain_ref),
                (in_shift_far, in_shift_ref),
                (w_gate_far, w_gate_ref),
                (out_gain_far, out_gain_ref),
                (out_shift_far, out_shift_ref),
                (w_out_far, w_out_ref),
            )
        )
    ]
    for load in loads:
        load.start()
    barrier = pltpu.get_barrier_semaphore()

    def greet(s):
        pl.semaphore_signal(barrier, inc=1, device_id=device(part_base + s), device_id_type=MESH)

    repeat(members - 1, lambda d: greet(lax.rem(my_slot + d + 1, members)))

    loads[1].wait()
    w_flat = w_proj_ref[...].astype(F32).T.astype(BF16)
    for h in range(chunks):
        size = members * sizes[h]
        for n in range(4):
            w_turned[pl.ds(4 * bases[h] + n * size, size), :] = w_flat[
                n * hidden + bases[h] : n * hidden + bases[h] + size
            ]
    for n in (0, 2, 3):
        loads[n].wait()
    def normalize(kg):
        values = x_ref[pl.ds(kg * WIDE, WIDE)].astype(F32)
        centred = values - jnp.mean(values, axis=-1, keepdims=True)
        variance = jnp.mean(centred * centred, axis=-1, keepdims=True)
        slabs_near[kg][...] = (
            centred * lax.rsqrt(variance + 1e-05) * in_gain_ref[...].reshape(1, 1, width)
            + in_shift_ref[...].reshape(1, 1, width)
        ).reshape(WIDE * local_i, width)

    first_slab = lax.rem(my_row, part_rows) * deep
    my_turn = lax.rem(my_other, SUB)

    def edge_block(kg, ig):
        return jnp.concatenate(
            [
                slabs_near[kg][
                    pl.ds(
                        ig * SUB
                        + lax.rem(p + SUB * part_rows * deep - first_slab - kg, SUB),
                        WIDE,
                        stride=local_i,
                    ),
                    :,
                ]
                for p in range(SUB)
            ],
            axis=0,
        ).astype(BF16)

    def place(pair, first, p):
        i = lax.rem(p + 2 * SUB - my_turn, 2 * SUB)
        return (2 * pair + lax.div(i, SUB)) * local_i + first * SUB + lax.rem(i, SUB)

    def gate_block(pair, first, second):
        return jnp.concatenate(
            [
                normed[pl.ds(pl.multiple_of(place(pair, first, p) * local_i + second * SUB, SUB), SUB), :]
                for p in range(2 * SUB)
            ],
            axis=0,
        ).astype(BF16)

    def project(h):
        each = sizes[h]
        part_hidden = members * each
        span1 = each * 2 * tiles
        for t in range(tiles):
            if h == 0:
                if t % groups == 0:
                    normalize(t // groups)
                blocks[t] = edge_block(t // groups, t % groups)
            projected = dot(w_turned[pl.ds(4 * bases[h], 4 * part_hidden), :], blocks[t], 1, 1)
            for side in range(2):
                gates = projected[2 * side * part_hidden : (2 * side + 1) * part_hidden]
                edges = projected[(2 * side + 1) * part_hidden : (2 * side + 2) * part_hidden]
                packed[pl.ds(side * tiles + t, part_hidden, stride=2 * tiles), :] = (
                    (0.5 * jnp.tanh(0.5 * gates) + 0.5) * edges
                )

        def pack(s):
            send1[h][s] = packed[pl.ds(s * span1, span1), :].reshape(send1[h].shape[1:]).astype(BF16)

        repeat(members, pack)

    def exchange(h, n, sent, kept, source, target, p):
        return pltpu.make_async_remote_copy(
            src_ref=sent[h].at[source],
            dst_ref=kept[h].at[target],
            send_sem=sems.at[n, h],
            recv_sem=sems.at[n + 1, h],
            device_id=device(p),
            device_id_type=MESH,
        )

    def copy1(h, s):
        return exchange(h, 0, send1, recv1, s, my_slot, part_base + s)

    def all1(h):
        some = pl.ds(0, members - 1)
        return exchange(h, 0, send1, recv1, some, some, me)

    def copy2(h, p):
        return exchange(h, 2, send2, recv2, p, me, p)

    def all2(h):
        some = pl.ds(0, count - 1)
        return exchange(h, 2, send2, recv2, some, some, me)

    def stop(k):
        other = jnp.where(k > my_row, k, k - 1)
        return jnp.where((k == 0) | (k == rows), my_row, other)

    def route(d):
        k, e = (d + 1) // others, (d + 1) % others
        row = jnp.where(my_other + e >= others, stop(k + 1), stop(k))
        return row * others + lax.rem(my_other + e, others)

    routes = [route(d) for d in range(count - 1 if count <= UNROLL else 0)]
    partner = lax.rem(me + count // 2, count)

    def send_off(h):
        project(h)
        if h == 0:
            pl.semaphore_wait(barrier, members - 1 + my_part)

            @pl.when(my_part == 0)
            def _():
                pl.semaphore_signal(barrier, inc=1, device_id=device(partner), device_id_type=MESH)

        repeat(members - 1, lambda d: copy1(h, lax.rem(my_slot + members - 1 - d, members)).start())
        recv1[h][my_slot] = send1[h][my_slot]
        if h == 0:

            @pl.when(my_part == 1)
            def _():
                pl.semaphore_signal(ready, inc=1, device_id=device(partner), device_id_type=MESH)

    for h in range(ahead):
        send_off(h)
    for kg in range(deep):
        normed[pl.ds(kg * WIDE * local_i, WIDE * local_i), :] = slabs_near[kg][...]
    for load in loads[4:]:
        load.wait()
    for t in range(pairs * groups * groups):
        pair, rest = t // (groups * groups), t % (groups * groups)
        gating[t] = jax.nn.sigmoid(
            dot(gate_block(pair, rest // groups, rest % groups), w_gate_ref[...], 1, 0)
        )
    lane = lax.broadcasted_iota(jnp.int32, (line, LANES), 1)
    small_lane = lax.broadcasted_iota(jnp.int32, (SUB, LANES), 1)

    def order(values):
        turned[...] = values
        return jnp.concatenate(
            [
                turned[pl.ds(bases[h] + c, members, stride=sizes[h]), :]
                for h in range(chunks)
                for c in range(sizes[h])
            ],
            axis=0,
        )

    def middle(h):
        each = sizes[h]
        span1 = each * 2 * tiles
        all1(h).wait_recv()

        def take(s):
            gathered[pl.ds(s * span1, span1), :] = recv1[h][s].astype(F32).reshape(span1, LANES)

        repeat(members, take)
        half = SUB * line // 2
        for c in range(each):
            for side in range(2):
                for kt in range(slab_tiles):
                    arrays = []
                    for kb in range(kt * SUB, kt * SUB + SUB):
                        if kb >= slabs:
                            arrays.append(None)
                            continue
                        start = (
                            (kb // deep) * others * span1
                            + (c * 2 + side) * tiles
                            + (kb % deep) * groups
                        )
                        arrays.append(
                            jnp.concatenate(
                                [
                                    gathered[pl.ds(start + g, others, stride=span1), :]
                                    for g in range(groups)
                                ],
                                axis=0,
                            )
                        )
                    for i, found in enumerate(gather_blocks(arrays, WIDE, lane)):
                        turned_back = pltpu.roll(found, LANES - i * WIDE, 1) if i else found
                        if side == 0:
                            left_rows[kt, pl.ds(i * line, line), :] = turned_back
                        else:
                            right_rows[kt, pl.ds(i, line, stride=SUB), :] = turned_back
            left = jnp.concatenate(
                [left_rows[kt, pl.ds(b, half, stride=2), :] for b in range(2) for kt in range(slab_tiles)],
                axis=1,
            ).astype(BF16)
            wide = SUB * SUB

            def multiply(j, c=c, left=left):
                right = jnp.concatenate(
                    [right_rows[kt, pl.ds(j * wide, wide), :] for kt in range(slab_tiles)], axis=1
                ).astype(BF16)
                empty = jnp.zeros_like(right)
                both = jnp.concatenate(
                    [jnp.concatenate([right, empty], axis=1), jnp.concatenate([empty, right], axis=1)],
                    axis=0,
                )
                planes[j, pl.ds(c, half, stride=each), :] = dot(left, both, 1, 1)

            repeat(line // SUB, multiply)

        stretch = groups * rows * pairs * each
        unit = pairs * each

        def flatten(j):
            g, q = (j // (others // SUB), j % (others // SUB)) if isinstance(j, int) else (
                lax.div(j, others // SUB),
                lax.rem(j, others // SUB),
            )
            for part in range(stretch // SUB):
                arrays = [planes[j, pl.ds(i * stretch + part * SUB, SUB), :] for i in range(SUB)]
                arrays = [pltpu.roll(a, i * SUB, 1) if i else a for i, a in enumerate(arrays)]
                flat = gather_blocks(arrays, SUB, small_lane)
                for n in range(SUB // unit):
                    where = part * (SUB // unit) + n
                    first, r = where // rows, where % rows
                    for o in range(SUB):
                        send2[h][r * others + q * SUB + o, g * groups + first] = flat[o][
                            n * unit : (n + 1) * unit
                        ].astype(BF16)

        repeat(line // SUB, flatten)
        if h == 0:

            @pl.when(my_part == 0)
            def _():
                pl.semaphore_wait(ready, 1)

        repeat(count - 1, lambda d: copy2(h, routes[d] if isinstance(d, int) else route(d)).start())
        recv2[h][me] = send2[h][me]

    for h in range(chunks):
        middle(h)
        if h + ahead < chunks:
            send_off(h + ahead)
    out_gain = order(jnp.broadcast_to(out_gain_ref[...].reshape(1, hidden), (LANES, hidden)).T)
    out_shift = order(jnp.broadcast_to(out_shift_ref[...].reshape(1, hidden), (LANES, hidden)).T)
    w_out = order(w_out_ref[...].astype(F32)).astype(BF16)
    for h in range(chunks):
        all2(h).wait_recv()
        span2 = spots * pairs * sizes[h]

        def take2(s, h=h, span2=span2):
            total = recv2[h][s].astype(F32)
            for part in range(1, parts):
                total = total + recv2[h][part * members + s].astype(F32)
            start = bases[h] * spots * pairs + s * span2
            gathered2[pl.ds(start, span2), :] = total.reshape(span2, LANES)

        repeat(members, take2)

    for t in range(pairs * groups * groups):
        pair, rest = t // (groups * groups), t % (groups * groups)
        first, second = rest // groups, rest % groups
        spot = (second * groups + first) * pairs + pair
        product = jnp.concatenate(
            [
                gathered2[
                    pl.ds(
                        bases[h] * spots * pairs + spot * sizes[h] + c,
                        members,
                        stride=spots * pairs * sizes[h],
                    ),
                    :,
                ]
                for h in range(chunks)
                for c in range(sizes[h])
            ],
            axis=0,
        )
        spread_out = product - jnp.mean(product, axis=0, keepdims=True)
        moment = jnp.mean(spread_out * spread_out, axis=0, keepdims=True)
        product_norm = (spread_out * lax.rsqrt(moment + 1e-05) * out_gain + out_shift).astype(BF16)
        update = (gating[t] * dot(product_norm, w_out, 0, 0)).astype(BF16)
        for p in range(2 * SUB):
            out_ref[place(pair, first, p), pl.ds(second * SUB, SUB), :] = update[p * SUB : (p + 1) * SUB]

    for h in range(chunks):
        all1(h).wait_send()
        all2(h).wait_send()


def per_device(mesh_sizes, pair_input, in_gain, in_shift, w_proj, w_gate, out_gain, out_shift, w_out):
    rows, cols, depths = mesh_sizes
    parts = 2
    others = cols * depths
    count = rows * others
    local_k, local_i, width = pair_input.shape
    hidden = w_out.shape[0]
    members = count // parts
    own = hidden // members
    sizes = SIZES if sum(SIZES) == own else (own // 2, own // 2)
    groups = local_i // SUB
    tiles = local_k * local_i // LANES
    most = max(sizes)
    line = groups * others
    pairs = local_k // local_i // 2
    spots = groups * groups
    slab_tiles = -(-(rows // parts * local_k) // LANES)
    operands = (
        pair_input,
        w_proj,
        in_gain.reshape(1, -1),
        in_shift.reshape(1, -1),
        w_gate,
        out_gain.reshape(1, -1),
        out_shift.reshape(1, -1),
        w_out,
    )

    def box1(each):
        tall = next(n for n in (SUB, 4, 2, 1) if each * 2 * tiles % n == 0)
        return pltpu.VMEM((members, each * 2 * tiles // tall, tall, LANES), BF16)

    def box2(each):
        return pltpu.VMEM((count, spots, pairs * each, LANES), BF16)

    scratch = [
        *(pltpu.VMEM(a.shape, a.dtype) for a in operands),
        pltpu.SemaphoreType.DMA((len(operands),)),
        pltpu.SemaphoreType.REGULAR,
        pltpu.VMEM((local_k * local_i, width), F32),
        pltpu.VMEM(w_proj.shape[::-1], BF16),
        pltpu.VMEM((tiles, LANES, width), BF16),
        pltpu.VMEM((tiles, LANES, width), F32),
        pltpu.VMEM((members * most * 2 * tiles, LANES), F32),
        pltpu.VMEM((members * most * 2 * tiles, LANES), F32),
        pltpu.VMEM((slab_tiles, SUB * line, LANES), F32),
        pltpu.VMEM((slab_tiles, SUB * line, LANES), F32),
        pltpu.VMEM((line // SUB, SUB * line // 2 * most, LANES), F32),
        pltpu.VMEM((hidden * spots * pairs, LANES), F32),
        pltpu.VMEM((hidden, LANES), F32),
        pltpu.SemaphoreType.DMA((4, len(sizes))),
        *(box(each) for box in (box1, box1, box2, box2) for each in sizes),
        *(pltpu.VMEM((WIDE * local_i, width), F32) for _ in range(local_k // WIDE)),
    ]
    return pl.pallas_call(
        functools.partial(kernel, (rows, cols, depths, parts, sizes, min(AHEAD, len(sizes)))),
        out_shape=pltpu.VMEM(pair_input.shape, BF16),
        in_specs=[pl.BlockSpec(memory_space=pltpu.HBM)] * len(operands),
        out_specs=pl.BlockSpec(memory_space=pltpu.VMEM),
        scratch_shapes=scratch,
        compiler_params=pltpu.CompilerParams(
            collective_id=0, has_side_effects=True, vmem_limit_bytes=60_000_000
        ),
    )(*(pltpu.with_memory_space_constraint(a, pltpu.HBM) for a in operands))


def solution(mesh):
    sizes = (mesh.shape["row"], mesh.shape["col"], mesh.shape["depth"])
    placed = (P("row", ("col", "depth"), None), P(), P(), P(), P(), P(), P(), P())
    return jax.shard_map(
        functools.partial(per_device, sizes),
        mesh=mesh,
        in_specs=placed,
        out_specs=P("row", ("col", "depth"), None),
        check_vma=False,
    )
```
